32 devices in a mesh: dp: 1 (over z), tp: 4 (over y), sp: 8 (over x, core).
Axes of the slice: x: 4, y: 4, z: 1, core: 2. Of those that a mesh axis runs over, the one named last changes fastest.
The devices are a block of a 4x4x8 slice.
Arguments:
- tokens: bfloat16 [64, 3840], P('dp')
- positions: int32 [64], P('dp')
- cache_k: bfloat16 [64, 1024, 8, 256], P('dp', 'sp', 'tp')
- cache_v: bfloat16 [64, 1024, 8, 256], P('dp', 'sp', 'tp')
- attn_gain: bfloat16 [3840], replicated
- w_q: bfloat16 [3840, 4096], P(None, 'tp')
- w_k: bfloat16 [3840, 2048], P(None, 'tp')
- w_v: bfloat16 [3840, 2048], P(None, 'tp')
- w_o: bfloat16 [4096, 3840], P('tp')
- mlp_gain: bfloat16 [3840], replicated
- w_gate: bfloat16 [3840, 15360], P(None, 'tp')
- w_up: bfloat16 [3840, 15360], P(None, 'tp')
- w_down: bfloat16 [15360, 3840], P('tp')
Outputs:
- output 1: bfloat16 [64, 3840], P('dp')
- output 2: bfloat16 [64, 1024, 8, 256], P('dp', 'sp', 'tp')
- output 3: bfloat16 [64, 1024, 8, 256], P('dp', 'sp', 'tp')
All inputs are finite; a program needn't handle non-finite values.
Results may differ from the reference program's by a relative error of at most 0.00836772.
Values sent between devices are 32-bit elements.
A program may use at most 768 MiB of HBM per device.

```python
import math
import jax
import jax.numpy as jnp
from jax import lax

BATCH = 64
MODEL_DIM = 3840
HEADS = 16
KV_HEADS = 8
HEAD_DIM = 256
MLP_DIM = 15360
SLOTS = 1024
GROUP = HEADS // KV_HEADS
POS_LIMIT = 8 * SLOTS
LOG_SLOTS = int(math.log2(SLOTS))
NORM_EPS = 1e-5
ROPE_THETA = 10000.0
KEY_STD = math.sqrt(math.log(SLOTS / 8.0))
VALUE_STD = 1.5


def draw_positions(key):
    rank_key, scale_key, young_key, old_key = jax.random.split(key, 4)
    order = jax.random.permutation(rank_key, BATCH)
    is_young = order < BATCH // 2
    exponent = jax.random.randint(scale_key, (BATCH,), 0, LOG_SLOTS + 1)
    limit = jnp.minimum(jnp.left_shift(jnp.ones_like(exponent), exponent), SLOTS)
    young_pos = jax.random.randint(young_key, (BATCH,), 0, limit)
    old_pos = jax.random.randint(old_key, (BATCH,), SLOTS, POS_LIMIT)
    return jnp.where(is_young, young_pos, old_pos).astype(jnp.int32)


def normal_matrix(key, rows, columns, scale):
    return (jax.random.normal(key, (rows, columns), jnp.float32) * scale).astype(jnp.bfloat16)


def normal_gain(key):
    return (1.0 + 0.3 * jax.random.normal(key, (MODEL_DIM,), jnp.float32)).astype(jnp.bfloat16)


def setup_inputs(seed: int = 0, part: int = 0) -> dict:
    base_key = jax.random.key(seed)
    part_keys = jax.random.split(jax.random.fold_in(base_key, part), 4)
    weight_keys = jax.random.split(base_key, 9)
    cache_shape = (BATCH, SLOTS, KV_HEADS, HEAD_DIM)
    query_width = HEADS * HEAD_DIM
    kv_width = KV_HEADS * HEAD_DIM
    tokens = jax.random.normal(part_keys[0], (BATCH, MODEL_DIM), jnp.float32).astype(jnp.bfloat16)
    positions = draw_positions(part_keys[1])
    cache_k = (KEY_STD * jax.random.normal(part_keys[2], cache_shape, jnp.float32)).astype(jnp.bfloat16)
    cache_v = (VALUE_STD * jax.random.normal(part_keys[3], cache_shape, jnp.float32)).astype(jnp.bfloat16)
    return {
        "tokens": tokens,
        "positions": positions,
        "cache_k": cache_k,
        "cache_v": cache_v,
        "attn_gain": normal_gain(weight_keys[0]),
        "w_q": normal_matrix(weight_keys[1], MODEL_DIM, query_width, MODEL_DIM ** -0.5),
        "w_k": normal_matrix(weight_keys[2], MODEL_DIM, kv_width, KEY_STD * MODEL_DIM ** -0.5),
        "w_v": normal_matrix(weight_keys[3], MODEL_DIM, kv_width, VALUE_STD * MODEL_DIM ** -0.5),
        "w_o": normal_matrix(weight_keys[4], query_width, MODEL_DIM, query_width ** -0.5),
        "mlp_gain": normal_gain(weight_keys[5]),
        "w_gate": normal_matrix(weight_keys[6], MODEL_DIM, MLP_DIM, MODEL_DIM ** -0.5),
        "w_up": normal_matrix(weight_keys[7], MODEL_DIM, MLP_DIM, MODEL_DIM ** -0.5),
        "w_down": normal_matrix(weight_keys[8], MLP_DIM, MODEL_DIM, MLP_DIM ** -0.5),
    }


def rms_norm(values, gain):
    wide = values.astype(jnp.float32)
    inv_rms = lax.rsqrt(jnp.mean(wide * wide, axis=-1, keepdims=True) + NORM_EPS)
    return (wide * inv_rms * gain.astype(jnp.float32)).astype(jnp.bfloat16)


def rope_tables(positions):
    frequencies = ROPE_THETA ** (-2.0 * jnp.arange(HEAD_DIM // 2, dtype=jnp.float32) / HEAD_DIM)
    angles = positions.astype(jnp.float32)[:, None] * frequencies[None, :]
    return jnp.cos(angles)[:, None, :], jnp.sin(angles)[:, None, :]


def apply_rope(vectors, cos_table, sin_table):
    half = vectors.shape[-1] // 2
    first = vectors[..., :half]
    second = vectors[..., half:]
    return jnp.concatenate([first * cos_table - second * sin_table, second * cos_table + first * sin_table], axis=-1)


def reference(tokens, positions, cache_k, cache_v, attn_gain, w_q, w_k, w_v, w_o, mlp_gain, w_gate, w_up, w_down):
    normed = rms_norm(tokens, attn_gain)
    cos_table, sin_table = rope_tables(positions)
    q_lin = jnp.dot(normed, w_q, preferred_element_type=jnp.float32).reshape(BATCH, HEADS, HEAD_DIM)
    k_lin = jnp.dot(normed, w_k, preferred_element_type=jnp.float32).reshape(BATCH, KV_HEADS, HEAD_DIM)
    v_new = jnp.dot(normed, w_v, preferred_element_type=jnp.float32).astype(jnp.bfloat16).reshape(BATCH, KV_HEADS, HEAD_DIM)
    q_rot = apply_rope(q_lin, cos_table, sin_table).astype(jnp.bfloat16)
    k_rot = apply_rope(k_lin, cos_table, sin_table).astype(jnp.bfloat16)
    slot_ids = jnp.arange(SLOTS)
    hit_mask = (slot_ids[None, :] == (positions % SLOTS)[:, None])[:, :, None, None]
    new_k = jnp.where(hit_mask, k_rot[:, None], cache_k)
    new_v = jnp.where(hit_mask, v_new[:, None], cache_v)

    def attend_one(item):
        q_seq, k_seq, v_seq, pos_one = item
        query = q_seq.astype(jnp.float32).reshape(KV_HEADS, GROUP, HEAD_DIM)
        scores = jnp.einsum("kgd,skd->kgs", query, k_seq.astype(jnp.float32)) / math.sqrt(HEAD_DIM)
        valid = (pos_one >= SLOTS - 1) | (slot_ids <= pos_one)
        scores = jnp.where(valid[None, None, :], scores, -jnp.inf)
        weights = jax.nn.softmax(scores, axis=-1)
        return jnp.einsum("kgs,skd->kgd", weights, v_seq.astype(jnp.float32)).reshape(HEADS, HEAD_DIM)

    attended = lax.map(attend_one, (q_rot, new_k, new_v, positions))
    attended = attended.reshape(BATCH, HEADS * HEAD_DIM).astype(jnp.bfloat16)
    attn_proj = jnp.dot(attended, w_o, preferred_element_type=jnp.float32)
    hidden = (tokens.astype(jnp.float32) + attn_proj).astype(jnp.bfloat16)
    normed_mlp = rms_norm(hidden, mlp_gain)
    gate_proj = jnp.dot(normed_mlp, w_gate, preferred_element_type=jnp.float32)
    up_proj = jnp.dot(normed_mlp, w_up, preferred_element_type=jnp.float32)
    activated = (jax.nn.silu(gate_proj) * up_proj).astype(jnp.bfloat16)
    mlp_down = jnp.dot(activated, w_down, preferred_element_type=jnp.float32)
    layer_out = (hidden.astype(jnp.float32) + mlp_down).astype(jnp.bfloat16)
    return (layer_out, new_k, new_v)
```

```python
import functools, math
import jax, jax.numpy as jnp, numpy as np
from jax import lax
from jax.experimental import pallas as pl
from jax.experimental.pallas import tpu as pltpu

NORM_EPS = 1e-5
ROPE_THETA = 10000.0
GRP = 8
KSTEP = 768


def attend_kernel(sp_size, tok_ref, pos_ref, posv_ref, freq_ref, gain_ref, wq_hbm, wk_hbm, wv_hbm, ck_hbm, cv_hbm,
                  part_ref, nk_hbm, nv_hbm,
                  wq, wk, wv, kbuf, vbuf, acc, normed, qrows, knew, vnew, wsem, csem, osem):
    rows, width = tok_ref.shape
    slots_local = kbuf.shape[1]
    kv_heads = kbuf.shape[2]
    head = kbuf.shape[3]
    q_cols, k_cols = wq.shape[1], wk.shape[1]
    heads = q_cols // head
    half = head // 2
    slots = slots_local * sp_size
    my_first = lax.axis_index("sp") * slots_local
    groups = rows // GRP
    ksteps = width // KSTEP

    def wcopies(c):
        sl = pl.ds(pl.multiple_of(c * KSTEP, KSTEP), KSTEP)
        return [pltpu.make_async_copy(src.at[sl], dst.at[sl], wsem.at[i, c])
                for i, (src, dst) in enumerate(((wq_hbm, wq), (wk_hbm, wk), (wv_hbm, wv)))]

    def ccopies(g):
        sl = pl.ds(g * GRP, GRP)
        return [pltpu.make_async_copy(ck_hbm.at[sl], kbuf.at[sl], csem.at[0, g]),
                pltpu.make_async_copy(cv_hbm.at[sl], vbuf.at[sl], csem.at[1, g])]

    def ocopies(g):
        sl = pl.ds(g * GRP, GRP)
        return [pltpu.make_async_copy(kbuf.at[sl], nk_hbm.at[sl], osem.at[0, g]),
                pltpu.make_async_copy(vbuf.at[sl], nv_hbm.at[sl], osem.at[1, g])]

    for c in range(ksteps):
        for cp in wcopies(c):
            cp.start()
    for g in range(groups):
        for cp in ccopies(g):
            cp.start()

    wide = tok_ref[...].astype(jnp.float32)
    inv = lax.rsqrt(jnp.mean(wide * wide, axis=-1, keepdims=True) + NORM_EPS)
    normed[...] = (wide * inv * gain_ref[...].astype(jnp.float32)).astype(jnp.bfloat16)
    angles = posv_ref[...].astype(jnp.float32) * freq_ref[...]
    cos, sin = jnp.cos(angles), jnp.sin(angles)
    acc[...] = jnp.zeros_like(acc)

    @pl.loop(0, ksteps)
    def _(c):
        for cp in wcopies(c):
            cp.wait()
        sl = pl.ds(pl.multiple_of(c * KSTEP, KSTEP), KSTEP)
        lhs = normed[:, sl]
        for w, off, cols in ((wq, 0, q_cols), (wk, q_cols, k_cols), (wv, q_cols + k_cols, k_cols)):
            acc[:, off:off + cols] += jnp.dot(lhs, w[sl, :], preferred_element_type=jnp.float32)

    def rope(off):
        a = acc[:, off:off + half]
        b = acc[:, off + half:off + head]
        return jnp.concatenate([a * cos - b * sin, b * cos + a * sin], axis=-1)

    for h in range(heads):
        q = rope(h * head).astype(jnp.bfloat16).astype(jnp.float32)
        qrows[0, pl.ds(h, rows, stride=heads), :] = q[:, :half]
        qrows[1, pl.ds(h, rows, stride=heads), :] = q[:, half:]
    for h in range(kv_heads):
        knew[:, h, :] = rope(q_cols + h * head)
        off = q_cols + k_cols + h * head
        vnew[:, h, :] = acc[:, off:off + head]

    pair = 8 // heads
    merged = slots_local * kv_heads
    lane = lax.broadcasted_iota(jnp.int32, (8, merged), 1)
    row = lax.broadcasted_iota(jnp.int32, (8, merged), 0)
    lane_slot = my_first + lane // kv_heads
    same_head = (lane % kv_heads) == ((row % heads) // (heads // kv_heads))
    scale = 1.0 / math.sqrt(head)
    stat_lane = lax.broadcasted_iota(jnp.int32, (8, 128), 1)
    n_pairs = GRP // pair
    span = 128 // (2 * n_pairs)

    @pl.loop(0, groups)
    def _(g):
        for cp in ccopies(g):
            cp.wait()
        for i in range(GRP):
            b = g * GRP + i
            local = pos_ref[b] % slots - my_first

            @pl.when((local >= 0) & (local < slots_local))
            def _():
                kbuf[b, local] = knew[b].astype(jnp.bfloat16)
                vbuf[b, local] = vnew[b].astype(jnp.bfloat16)
        for cp in ocopies(g):
            cp.start()
        stat = jnp.zeros((8, 128), jnp.float32)
        for j in range(n_pairs):
            b0 = g * GRP + j * pair
            q_at = pl.ds(pl.multiple_of(b0 * heads, 8), 8)
            q8 = jnp.concatenate([qrows[0, q_at, :], qrows[1, q_at, :]], axis=-1).astype(jnp.bfloat16)
            s = None
            lim = None
            for i in range(pair):
                kk = kbuf[b0 + i].reshape(merged, head)
                si = lax.dot_general(q8, kk, (((1,), (1,)), ((), ())), preferred_element_type=jnp.float32)
                li = jnp.minimum(pos_ref[b0 + i], slots - 1)
                s = si if s is None else jnp.where(row < i * heads, s, si)
                lim = jnp.full((8, merged), li, jnp.int32) if lim is None else jnp.where(row < i * heads, lim, li)
            valid = same_head & (lane_slot <= lim)
            s = jnp.where(valid, s * scale, -jnp.inf)
            top = jnp.max(s, axis=-1, keepdims=True)
            safe = jnp.where(top == -jnp.inf, 0.0, top)
            p = jnp.exp(s - safe)
            total = jnp.sum(p, axis=-1, keepdims=True)
            out = None
            for i in range(pair):
                vv = vbuf[b0 + i].reshape(merged, head)
                mine = (row >= i * heads) & (row < (i + 1) * heads)
                oi = jnp.dot(jnp.where(mine, p, 0.0).astype(jnp.bfloat16), vv, preferred_element_type=jnp.float32)
                out = oi if out is None else out + oi
            part_ref[g, j * 8:(j + 1) * 8, :] = out
            lo = 2 * j * span
            stat = jnp.where((stat_lane >= lo) & (stat_lane < lo + span), top, stat)
            stat = jnp.where((stat_lane >= lo + span) & (stat_lane < lo + 2 * span), total, stat)
        part_ref[g, n_pairs * 8:, :128] = stat
        part_ref[g, n_pairs * 8:, 128:] = stat

    for g in range(groups):
        for cp in ocopies(g):
            cp.wait()


def attend(sp_size, tokens, positions, cache_k, cache_v, gain, w_q, w_k, w_v):
    rows, width = tokens.shape
    _, slots_local, kv_heads, head = cache_k.shape
    heads = w_q.shape[1] // head
    freq = jnp.asarray((np.float32(ROPE_THETA) ** (np.float32(-2.0) * np.arange(head // 2, dtype=np.float32) / np.float32(head))).astype(np.float32))[None, :]
    groups = rows // GRP
    chunk_rows = GRP * heads + 8
    any_spec = pl.BlockSpec(memory_space=pl.ANY)
    vm = pl.BlockSpec(memory_space=pltpu.VMEM)
    qkv_cols = w_q.shape[1] + 2 * w_k.shape[1]
    bf = jnp.bfloat16
    return pl.pallas_call(
        functools.partial(attend_kernel, sp_size),
        out_shape=(jax.ShapeDtypeStruct((groups, chunk_rows, head), jnp.float32),
                   jax.ShapeDtypeStruct(cache_k.shape, bf), jax.ShapeDtypeStruct(cache_v.shape, bf)),
        in_specs=[vm, pl.BlockSpec(memory_space=pltpu.SMEM), vm, vm, vm] + [any_spec] * 5,
        out_specs=(vm, any_spec, any_spec),
        scratch_shapes=[
            pltpu.VMEM(w_q.shape, bf), pltpu.VMEM(w_k.shape, bf), pltpu.VMEM(w_v.shape, bf),
            pltpu.VMEM(cache_k.shape, bf), pltpu.VMEM(cache_v.shape, bf),
            pltpu.VMEM((rows, qkv_cols), jnp.float32), pltpu.VMEM((rows, width), bf),
            pltpu.VMEM((2, rows * heads, head // 2), jnp.float32),
            pltpu.VMEM((rows, kv_heads, head), jnp.float32), pltpu.VMEM((rows, kv_heads, head), jnp.float32),
            pltpu.SemaphoreType.DMA((3, width // KSTEP)), pltpu.SemaphoreType.DMA((2, groups)), pltpu.SemaphoreType.DMA((2, groups)),
        ],
        compiler_params=pltpu.CompilerParams(vmem_limit_bytes=56 << 20),
        name="attend",
    )(tokens, positions, positions[:, None], freq, gain[None, :], w_q, w_k, w_v, cache_k, cache_v)


from jax.sharding import PartitionSpec as P


def rms_norm(values, gain):
    wide = values.astype(jnp.float32)
    inv_rms = lax.rsqrt(jnp.mean(wide * wide, axis=-1, keepdims=True) + NORM_EPS)
    return (wide * inv_rms * gain.astype(jnp.float32)).astype(jnp.bfloat16)


def solution(mesh):
    sp_size = mesh.shape["sp"]
    cache_spec = P("dp", "sp", "tp", None)
    row_spec = P("dp", None)
    col_spec = P(None, "tp")
    in_specs = (row_spec, P("dp"), cache_spec, cache_spec, P(None), col_spec, col_spec, col_spec, P("tp", None), P(None), col_spec, col_spec, P("tp", None))
    out_specs = (row_spec, cache_spec, cache_spec)

    def local_step(tokens, positions, cache_k, cache_v, attn_gain, w_q, w_k, w_v, w_o, mlp_gain, w_gate, w_up, w_down):
        rows = tokens.shape[0]
        head = cache_k.shape[3]
        heads = w_q.shape[1] // head
        part, new_k, new_v = attend(sp_size, tokens, positions, cache_k, cache_v, attn_gain, w_q, w_k, w_v)
        g = rows // GRP
        o = part[:, :GRP * heads, :].reshape(rows, heads, head)
        st = part[:, GRP * heads:, :128].reshape(g, 8, 8, 16)[..., 0]
        n_pairs = GRP * heads // 8
        st = st.reshape(g, 8, n_pairs, 2).transpose(3, 0, 2, 1).reshape(2, rows, heads)
        m, l = st[0], st[1]
        gm = lax.pmax(m, "sp")
        f = jnp.exp(m - gm)
        packed = jnp.concatenate([o * f[..., None], (l * f)[..., None]], axis=-1)
        total = lax.psum(packed, "sp")
        attended = (total[..., :head] / total[..., head:]).astype(jnp.bfloat16).reshape(rows, heads * head)
        attn_proj = lax.psum(jnp.dot(attended, w_o, preferred_element_type=jnp.float32), "tp")
        hidden = (tokens.astype(jnp.float32) + attn_proj).astype(jnp.bfloat16)
        normed_mlp = rms_norm(hidden, mlp_gain)
        gate_proj = jnp.dot(normed_mlp, w_gate, preferred_element_type=jnp.float32)
        up_proj = jnp.dot(normed_mlp, w_up, preferred_element_type=jnp.float32)
        activated = (jax.nn.silu(gate_proj) * up_proj).astype(jnp.bfloat16)
        mlp_down = lax.psum(jnp.dot(activated, w_down, preferred_element_type=jnp.float32), "tp")
        layer_out = (hidden.astype(jnp.float32) + mlp_down).astype(jnp.bfloat16)
        return layer_out, new_k, new_v

    return jax.shard_map(local_step, mesh=mesh, in_specs=in_specs, out_specs=out_specs, check_vma=False)
```

```python
import functools, math
import jax, jax.numpy as jnp, numpy as np
from jax import lax
from jax.experimental import pallas as pl
from jax.experimental.pallas import tpu as pltpu

NORM_EPS = 1e-5
ROPE_THETA = 10000.0
GRP = 8
KSTEP = 768


def attend_kernel(sp_size, tok_ref, pos_ref, posv_ref, freq_ref, gain_ref, wq_hbm, wk_hbm, wv_hbm, ck_hbm, cv_hbm,
                  part_ref, nk_hbm, nv_hbm,
                  wq, wk, wv, kbuf, vbuf, acc, normed, qrows, knew, vnew, wsem, csem, osem):
    rows, width = tok_ref.shape
    slots_local = kbuf.shape[1]
    kv_heads = kbuf.shape[2]
    head = kbuf.shape[3]
    q_cols, k_cols = wq.shape[1], wk.shape[1]
    heads = q_cols // head
    half = head // 2
    slots = slots_local * sp_size
    my_first = lax.axis_index("sp") * slots_local
    groups = rows // GRP
    ksteps = width // KSTEP

    def wcopies(c):
        sl = pl.ds(pl.multiple_of(c * KSTEP, KSTEP), KSTEP)
        return [pltpu.make_async_copy(src.at[sl], dst.at[sl], wsem.at[i, c])
                for i, (src, dst) in enumerate(((wq_hbm, wq), (wk_hbm, wk), (wv_hbm, wv)))]

    def ccopies(g):
        sl = pl.ds(g * GRP, GRP)
        return [pltpu.make_async_copy(ck_hbm.at[sl], kbuf.at[sl], csem.at[0, g]),
                pltpu.make_async_copy(cv_hbm.at[sl], vbuf.at[sl], csem.at[1, g])]

    def ocopies(g):
        sl = pl.ds(g * GRP, GRP)
        return [pltpu.make_async_copy(kbuf.at[sl], nk_hbm.at[sl], osem.at[0, g]),
                pltpu.make_async_copy(vbuf.at[sl], nv_hbm.at[sl], osem.at[1, g])]

    for c in range(ksteps):
        for cp in wcopies(c):
            cp.start()
    for g in range(groups):
        for cp in ccopies(g):
            cp.start()

    wide = tok_ref[...].astype(jnp.float32)
    inv = lax.rsqrt(jnp.mean(wide * wide, axis=-1, keepdims=True) + NORM_EPS)
    normed[...] = (wide * inv * gain_ref[...].astype(jnp.float32)).astype(jnp.bfloat16)
    angles = posv_ref[...].astype(jnp.float32) * freq_ref[...]
    cos, sin = jnp.cos(angles), jnp.sin(angles)
    acc[...] = jnp.zeros_like(acc)

    @pl.loop(0, ksteps)
    def _(c):
        for cp in wcopies(c):
            cp.wait()
        sl = pl.ds(pl.multiple_of(c * KSTEP, KSTEP), KSTEP)
        lhs = normed[:, sl]
        for w, off, cols in ((wq, 0, q_cols), (wk, q_cols, k_cols), (wv, q_cols + k_cols, k_cols)):
            acc[:, off:off + cols] += jnp.dot(lhs, w[sl, :], preferred_element_type=jnp.float32)

    def rope(off):
        a = acc[:, off:off + half]
        b = acc[:, off + half:off + head]
        return jnp.concatenate([a * cos - b * sin, b * cos + a * sin], axis=-1)

    for h in range(heads):
        q = rope(h * head).astype(jnp.bfloat16).astype(jnp.float32)
        qrows[0, pl.ds(h, rows, stride=heads), :] = q[:, :half]
        qrows[1, pl.ds(h, rows, stride=heads), :] = q[:, half:]
    for h in range(kv_heads):
        knew[:, h, :] = rope(q_cols + h * head)
        off = q_cols + k_cols + h * head
        vnew[:, h, :] = acc[:, off:off + head]

    pair = 8 // heads
    merged = slots_local * kv_heads
    lane = lax.broadcasted_iota(jnp.int32, (8, merged), 1)
    row = lax.broadcasted_iota(jnp.int32, (8, merged), 0)
    lane_slot = my_first + lane // kv_heads
    same_head = (lane % kv_heads) == ((row % heads) // (heads // kv_heads))
    scale = 1.0 / math.sqrt(head)
    stat_lane = lax.broadcasted_iota(jnp.int32, (8, 128), 1)
    n_pairs = GRP // pair
    span = 128 // (2 * n_pairs)

    @pl.loop(0, groups)
    def _(g):
        for cp in ccopies(g):
            cp.wait()
        for i in range(GRP):
            b = g * GRP + i
            local = pos_ref[b] % slots - my_first

            @pl.when((local >= 0) & (local < slots_local))
            def _():
                kbuf[b, local] = knew[b].astype(jnp.bfloat16)
                vbuf[b, local] = vnew[b].astype(jnp.bfloat16)
        for cp in ocopies(g):
            cp.start()
        stat = jnp.zeros((8, 128), jnp.float32)
        for j in range(n_pairs):
            b0 = g * GRP + j * pair
            q_at = pl.ds(pl.multiple_of(b0 * heads, 8), 8)
            q8 = jnp.concatenate([qrows[0, q_at, :], qrows[1, q_at, :]], axis=-1).astype(jnp.bfloat16)
            s = None
            lim = None
            for i in range(pair):
                kk = kbuf[b0 + i].reshape(merged, head)
                si = lax.dot_general(q8, kk, (((1,), (1,)), ((), ())), preferred_element_type=jnp.float32)
                li = jnp.minimum(pos_ref[b0 + i], slots - 1)
                s = si if s is None else jnp.where(row < i * heads, s, si)
                lim = jnp.full((8, merged), li, jnp.int32) if lim is None else jnp.where(row < i * heads, lim, li)
            valid = same_head & (lane_slot <= lim)
            s = jnp.where(valid, s * scale, -jnp.inf)
            top = jnp.max(s, axis=-1, keepdims=True)
            safe = jnp.where(top == -jnp.inf, 0.0, top)
            p = jnp.exp(s - safe)
            total = jnp.sum(p, axis=-1, keepdims=True)
            out = None
            for i in range(pair):
                vv = vbuf[b0 + i].reshape(merged, head)
                mine = (row >= i * heads) & (row < (i + 1) * heads)
                oi = jnp.dot(jnp.where(mine, p, 0.0).astype(jnp.bfloat16), vv, preferred_element_type=jnp.float32)
                out = oi if out is None else out + oi
            part_ref[g, j * 8:(j + 1) * 8, :] = out
            lo = 2 * j * span
            stat = jnp.where((stat_lane >= lo) & (stat_lane < lo + span), top, stat)
            stat = jnp.where((stat_lane >= lo + span) & (stat_lane < lo + 2 * span), total, stat)
        part_ref[g, n_pairs * 8:, :128] = stat
        part_ref[g, n_pairs * 8:, 128:] = stat

    for g in range(groups):
        for cp in ocopies(g):
            cp.wait()


def attend(sp_size, tokens, positions, cache_k, cache_v, gain, w_q, w_k, w_v):
    rows, width = tokens.shape
    _, slots_local, kv_heads, head = cache_k.shape
    heads = w_q.shape[1] // head
    freq = jnp.asarray((np.float32(ROPE_THETA) ** (np.float32(-2.0) * np.arange(head // 2, dtype=np.float32) / np.float32(head))).astype(np.float32))[None, :]
    groups = rows // GRP
    chunk_rows = GRP * heads + 8
    any_spec = pl.BlockSpec(memory_space=pl.ANY)
    vm = pl.BlockSpec(memory_space=pltpu.VMEM)
    qkv_cols = w_q.shape[1] + 2 * w_k.shape[1]
    bf = jnp.bfloat16
    return pl.pallas_call(
        functools.partial(attend_kernel, sp_size),
        out_shape=(jax.ShapeDtypeStruct((groups, chunk_rows, head), jnp.float32),
                   jax.ShapeDtypeStruct(cache_k.shape, bf), jax.ShapeDtypeStruct(cache_v.shape, bf)),
        in_specs=[vm, pl.BlockSpec(memory_space=pltpu.SMEM), vm, vm, vm] + [any_spec] * 5,
        out_specs=(vm, any_spec, any_spec),
        scratch_shapes=[
            pltpu.VMEM(w_q.shape, bf), pltpu.VMEM(w_k.shape, bf), pltpu.VMEM(w_v.shape, bf),
            pltpu.VMEM(cache_k.shape, bf), pltpu.VMEM(cache_v.shape, bf),
            pltpu.VMEM((rows, qkv_cols), jnp.float32), pltpu.VMEM((rows, width), bf),
            pltpu.VMEM((2, rows * heads, head // 2), jnp.float32),
            pltpu.VMEM((rows, kv_heads, head), jnp.float32), pltpu.VMEM((rows, kv_heads, head), jnp.float32),
            pltpu.SemaphoreType.DMA((3, width // KSTEP)), pltpu.SemaphoreType.DMA((2, groups)), pltpu.SemaphoreType.DMA((2, groups)),
        ],
        compiler_params=pltpu.CompilerParams(vmem_limit_bytes=56 << 20),
        name="attend",
    )(tokens, positions, positions[:, None], freq, gain[None, :], w_q, w_k, w_v, cache_k, cache_v)


MESH_ID = pl.DeviceIdType.MESH
CHUNK = 1024
CORES = 2


def finish_kernel(sp_size, tp_size, part_ref, tok_ref, gain_ref, wo_hbm, wg_hbm, wu_hbm, wd_hbm, out_ref,
                  wo, wg, wu, wd, crecv, att, toks, dsend, drecv, hbuf, normed, hidden_mlp, dpart, precv, gsum, g1recv, s1, g2recv, obuf,
                  wsem, csem, dsem, asem, bsem, psem, g1sem, g2sem):
    f32, bf = jnp.float32, jnp.bfloat16
    rows, width = tok_ref.shape
    n_x = sp_size // CORES
    heads_cols = wo.shape[0]
    mlp_cols = wg.shape[1]
    sp, tp = lax.axis_index("sp"), lax.axis_index("tp")
    x, core = sp // CORES, sp % CORES
    flip = 1 - core
    group = rows // sp_size

    def rc(src, dst, ssem, rsem, to_sp, to_tp):
        return pltpu.make_async_remote_copy(src_ref=src, dst_ref=dst, send_sem=ssem, recv_sem=rsem,
                                            device_id={"sp": to_sp, "tp": to_tp}, device_id_type=MESH_ID)

    blocks = wg_hbm.shape[1] // 128
    per = mlp_cols // 128
    first = jnp.minimum(sp * per, blocks - per)
    cols = pl.ds(pl.multiple_of(first * 128, 128), mlp_cols)
    loads = [pltpu.make_async_copy(wo_hbm, wo.at[:, pl.ds(0, width)], wsem.at[0]),
             pltpu.make_async_copy(wg_hbm.at[:, cols], wg, wsem.at[1]),
             pltpu.make_async_copy(wu_hbm.at[:, cols], wu, wsem.at[2]),
             pltpu.make_async_copy(wd_hbm.at[cols, :], wd.at[:, pl.ds(0, width)], wsem.at[3])]
    for cp in loads:
        cp.start()

    barrier = pltpu.get_barrier_semaphore()
    for k in range(1, sp_size):
        pl.semaphore_signal(barrier, inc=1, device_id={"sp": (sp + k) % sp_size, "tp": tp}, device_id_type=MESH_ID)
    for k in range(1, tp_size):
        pl.semaphore_signal(barrier, inc=1, device_id={"sp": sp, "tp": (tp + k) % tp_size}, device_id_type=MESH_ID)
    pl.semaphore_wait(barrier, sp_size + tp_size - 2)

    def part_copy(k):
        to = (sp + k) % sp_size
        return rc(part_ref.at[to], crecv.at[sp], csem.at[0, k - 1], csem.at[1, k - 1], to, tp)

    for k in range(1, sp_size):
        part_copy(k).start()
    pad = CHUNK * tp_size - width
    wo[:, width:] = jnp.zeros((heads_cols, pad), bf)
    wd[:, width:] = jnp.zeros((mlp_cols, pad), bf)
    for t in range(tp_size):
        w = min(CHUNK, width - t * CHUNK)
        toks[:, t, :, :w] = tok_ref[:, t * CHUNK:t * CHUNK + w].astype(f32).reshape(sp_size, group, w)
        if w < CHUNK:
            toks[:, t, :, w:] = jnp.zeros((sp_size, group, CHUNK - w), f32)
    crecv[sp] = part_ref[sp]
    for k in range(1, sp_size):
        src = (sp + sp_size - k) % sp_size
        rc(crecv.at[src], crecv.at[src], csem.at[0, k - 1], csem.at[1, k - 1], sp, tp).wait_recv()

    n_rows = part_ref.shape[1] - 8
    n_pairs = n_rows // 8
    span = 128 // (2 * n_pairs)
    head = part_ref.shape[2]
    heads = heads_cols // head
    stats = [crecv[i, n_rows:, :128] for i in range(sp_size)]
    top = functools.reduce(jnp.maximum, stats)
    factors = [jnp.exp(st - top) for st in stats]
    for j in range(n_pairs):
        lo = 2 * j * span
        num, den = None, None
        for i in range(sp_size):
            f = factors[i][:, lo:lo + 1]
            o = crecv[i, j * 8:(j + 1) * 8, :] * f
            l = stats[i][:, lo + span:lo + span + 1] * f
            num, den = (o, l) if num is None else (num + o, den + l)
        o = num / den
        att[0, j * 8:(j + 1) * 8, :] = o[:, :head // 2]
        att[1, j * 8:(j + 1) * 8, :] = o[:, head // 2:]
    attended = jnp.concatenate([att[half, pl.ds(h, group, stride=heads), :] for h in range(heads) for half in range(2)], axis=-1).astype(bf)

    loads[0].wait()

    def proj_copy(k):
        to = (tp + k) % tp_size
        return rc(dsend.at[to], drecv.at[k - 1], dsem.at[0, k - 1], dsem.at[1, k - 1], sp, to)

    order = (1, 3, 2) if tp_size == 4 else tuple(range(1, tp_size))
    for k in order + (0,):
        t = (tp + k) % tp_size
        dsend[t] = jnp.dot(attended, wo[:, pl.ds(pl.multiple_of(t * CHUNK, CHUNK), CHUNK)], preferred_element_type=f32)
        if k:
            proj_copy(k).start()
    total = toks[sp, tp] + dsend[tp]
    mine = dsend[tp]
    for k in order:
        rc(drecv.at[k - 1], drecv.at[k - 1], dsem.at[0, k - 1], dsem.at[1, k - 1], sp, tp).wait_recv()
        mine = mine + drecv[k - 1]
    hbuf[sp, tp] = (toks[sp, tp] + mine).astype(bf).astype(f32)

    def gather(buf, which):
        def chunk(s, t):
            return buf.at[s, t]

        def own_chunk(d_sp, d_tp, c, k, j):
            s = (d_sp + sp_size - CORES * (k * (1 - c) + j * c)) % sp_size
            t = (d_tp + tp_size - (k * c + j * (1 - c))) % tp_size
            return s, t

        def first_copy(k):
            return rc(chunk(sp, tp), chunk(sp, tp), asem.at[which, 0, k - 1], asem.at[which, 1, k - 1],
                      (sp + CORES * k * core) % sp_size, (tp + k * flip) % tp_size)

        def second_copy(k, j):
            s, t = own_chunk(sp, tp, core, 0, j)
            return rc(chunk(s, t), chunk(s, t), bsem.at[which, 0, k - 1, j], bsem.at[which, 1, k - 1, j],
                      (sp + CORES * k * flip) % sp_size, (tp + k * core) % tp_size)

        partner = sp + 1 - 2 * core

        def pair_copy(k, j):
            s, t = own_chunk(sp, tp, core, k, j)
            return rc(chunk(s, t), chunk(s, t), psem.at[which, 0, k, j], psem.at[which, 1, k, j], partner, tp)

        for k in order:
            first_copy(k).start()
        for k in order:
            second_copy(k, 0).start()
        pair_copy(0, 0).start()
        for j in order:
            s, t = own_chunk(sp, tp, core, 0, j)
            rc(chunk(s, t), chunk(s, t), asem.at[which, 0, j - 1], asem.at[which, 1, j - 1], sp, tp).wait_recv()
            for k in order:
                second_copy(k, j).start()
            pair_copy(0, j).start()
        for j in (0,) + order:
            for k in order:
                s, t = own_chunk(sp, tp, core, k, j)
                rc(chunk(s, t), chunk(s, t), bsem.at[which, 0, k - 1, j], bsem.at[which, 1, k - 1, j], sp, tp).wait_recv()
                pair_copy(k, j).start()
        for j in (0,) + order:
            for k in (0,) + order:
                s, t = own_chunk(partner, tp, flip, k, j)
                rc(chunk(s, t), chunk(s, t), psem.at[which, 0, k, j], psem.at[which, 1, k, j], sp, tp).wait_recv()
        for k in order:
            first_copy(k).wait_send()
            for j in range(tp_size):
                second_copy(k, j).wait_send()
        for k in range(n_x):
            for j in range(tp_size):
                pair_copy(k, j).wait_send()

    gather(hbuf, 0)

    square = None
    for t in range(tp_size):
        w = min(CHUNK, width - t * CHUNK)
        v = hbuf[:, t].reshape(rows, CHUNK)[:, :w]
        s = jnp.sum(v * v, axis=-1, keepdims=True)
        square = s if square is None else square + s
    inv = lax.rsqrt(square / width + NORM_EPS)
    for t in range(tp_size):
        w = min(CHUNK, width - t * CHUNK)
        v = hbuf[:, t].reshape(rows, CHUNK)[:, :w]
        normed[:, t * CHUNK:t * CHUNK + w] = (v * inv * gain_ref[:, t * CHUNK:t * CHUNK + w].astype(f32)).astype(bf)
    loads[1].wait()
    gate = jnp.dot(normed[...], wg[...], preferred_element_type=f32)
    loads[2].wait()
    up = jnp.dot(normed[...], wu[...], preferred_element_type=f32)
    block = first + lax.broadcasted_iota(jnp.int32, (rows, mlp_cols), 1) // 128
    hidden_mlp[...] = jnp.where(block >= sp * per, jax.nn.silu(gate) * up, 0.0).astype(bf)
    loads[3].wait()

    partner = sp + 1 - 2 * core

    def half_copy(t):
        return rc(dpart.at[:, flip, t], precv.at[:, t], psem.at[2, 0, 0, t], psem.at[2, 1, 0, t], partner, tp)

    steps = order + (0,)
    for i in steps:
        t = (tp + i) % tp_size
        part = jnp.dot(hidden_mlp[...], wd[:, pl.ds(pl.multiple_of(t * CHUNK, CHUNK), CHUNK)], preferred_element_type=f32)
        dpart[:, :, t] = part.reshape(n_x, CORES, group, CHUNK)
        half_copy(t).start()

    def x_copy(k, t):
        to = (x + k) % n_x
        return rc(gsum.at[to, t], g1recv.at[k - 1, t], g1sem.at[0, k - 1, t], g1sem.at[1, k - 1, t], CORES * to + core, tp)

    def y_copy(k, j):
        to = (tp + k) % tp_size
        return rc(gsum.at[j, to], g1recv.at[k - 1, j], g1sem.at[0, k - 1, j], g1sem.at[1, k - 1, j], sp, to)

    for i in steps:
        t = (tp + i) % tp_size
        rc(precv.at[:, t], precv.at[:, t], psem.at[2, 0, 0, t], psem.at[2, 1, 0, t], sp, tp).wait_recv()
        gsum[:, t] = dpart[:, core, t] + precv[:, t]

        @pl.when(core == 0)
        def _():
            for k in order:
                x_copy(k, t).start()

        if i:
            @pl.when(core == 1)
            def _():
                for j in range(n_x):
                    y_copy(i, j).start()

    b_own = tp * flip + x * core

    def b_copy(k):
        b = (b_own + k) % tp_size
        return rc(s1.at[b], g2recv.at[k - 1], g2sem.at[0, k - 1], g2sem.at[1, k - 1],
                  (sp + CORES * k * core) % sp_size, (tp + k * flip) % tp_size)

    for k in steps:
        b = (b_own + k) % tp_size
        acc = gsum[x * flip + b * core, b * flip + tp * core]
        for a in order:
            rc(g1recv.at[a - 1, b], g1recv.at[a - 1, b], g1sem.at[0, a - 1, b], g1sem.at[1, a - 1, b], sp, tp).wait_recv()
            acc = acc + g1recv[a - 1, b]
        s1[b] = acc
        if k:
            b_copy(k).start()
    acc = s1[b_own]
    for k in order:
        rc(g2recv.at[k - 1], g2recv.at[k - 1], g2sem.at[0, k - 1], g2sem.at[1, k - 1], sp, tp).wait_recv()
        acc = acc + g2recv[k - 1]
    obuf[sp, tp] = (hbuf[sp, tp] + acc).astype(bf).astype(f32)

    gather(obuf, 1)
    for t in range(tp_size):
        w = min(CHUNK, width - t * CHUNK)
        out_ref[:, t * CHUNK:t * CHUNK + w] = obuf[:, t].reshape(rows, CHUNK)[:, :w].astype(bf)

    for k in range(1, sp_size):
        part_copy(k).wait_send()
    for k in order:
        proj_copy(k).wait_send()
        b_copy(k).wait_send()
    for t in range(tp_size):
        half_copy(t).wait_send()

    @pl.when(core == 0)
    def _():
        for k in order:
            for t in range(tp_size):
                x_copy(k, t).wait_send()

    @pl.when(core == 1)
    def _():
        for k in order:
            for j in range(n_x):
                y_copy(k, j).wait_send()


def finish(sp_size, tp_size, part, tokens, gain, w_o, w_gate, w_up, w_down):
    rows, width = tokens.shape
    group = rows // sp_size
    n_x = sp_size // CORES
    blocks = w_gate.shape[1] // 128
    mlp_cols = -(-blocks // sp_size) * 128
    padded = CHUNK * tp_size
    f32, bf = jnp.float32, jnp.bfloat16
    any_spec = pl.BlockSpec(memory_space=pl.ANY)
    vm = pl.BlockSpec(memory_space=pltpu.VMEM)
    dma = pltpu.SemaphoreType.DMA
    head = part.shape[2]
    return pl.pallas_call(
        functools.partial(finish_kernel, sp_size, tp_size),
        out_shape=jax.ShapeDtypeStruct((rows, width), bf),
        in_specs=[vm, vm, vm] + [any_spec] * 4,
        out_specs=vm,
        scratch_shapes=[
            pltpu.VMEM((w_o.shape[0], padded), bf), pltpu.VMEM((width, mlp_cols), bf), pltpu.VMEM((width, mlp_cols), bf), pltpu.VMEM((mlp_cols, padded), bf),
            pltpu.VMEM(part.shape, f32), pltpu.VMEM((2, part.shape[1] - 8, head // 2), f32),
            pltpu.VMEM((sp_size, tp_size, group, CHUNK), f32),
            pltpu.VMEM((tp_size, group, CHUNK), f32), pltpu.VMEM((tp_size - 1, group, CHUNK), f32),
            pltpu.VMEM((sp_size, tp_size, group, CHUNK), f32),
            pltpu.VMEM((rows, width), bf), pltpu.VMEM((rows, mlp_cols), bf),
            pltpu.VMEM((n_x, CORES, tp_size, group, CHUNK), f32), pltpu.VMEM((n_x, tp_size, group, CHUNK), f32), pltpu.VMEM((n_x, tp_size, group, CHUNK), f32),
            pltpu.VMEM((3, tp_size, group, CHUNK), f32), pltpu.VMEM((tp_size, group, CHUNK), f32), pltpu.VMEM((3, group, CHUNK), f32),
            pltpu.VMEM((sp_size, tp_size, group, CHUNK), f32),
            dma((4,)), dma((2, sp_size - 1)), dma((2, tp_size - 1)), dma((2, 2, 3)), dma((2, 2, 3, tp_size)), dma((3, 2, n_x, tp_size)),
            dma((2, 3, tp_size)), dma((2, 3)),
        ],
        compiler_params=pltpu.CompilerParams(vmem_limit_bytes=56 << 20, collective_id=0, has_side_effects=True),
        name="finish",
    )(part, tokens, gain[None, :], w_o, w_gate, w_up, w_down)


from jax.sharding import PartitionSpec as P


def solution(mesh):
    sp_size, tp_size = mesh.shape["sp"], mesh.shape["tp"]
    cache_spec = P("dp", "sp", "tp", None)
    row_spec = P("dp", None)
    col_spec = P(None, "tp")
    in_specs = (row_spec, P("dp"), cache_spec, cache_spec, P(None), col_spec, col_spec, col_spec, P("tp", None), P(None), col_spec, col_spec, P("tp", None))
    out_specs = (row_spec, cache_spec, cache_spec)

    def local_step(tokens, positions, cache_k, cache_v, attn_gain, w_q, w_k, w_v, w_o, mlp_gain, w_gate, w_up, w_down):
        part, new_k, new_v = attend(sp_size, tokens, positions, cache_k, cache_v, attn_gain, w_q, w_k, w_v)
        layer_out = finish(sp_size, tp_size, part, tokens, mlp_gain, w_o, w_gate, w_up, w_down)
        return layer_out, new_k, new_v

    return jax.shard_map(local_step, mesh=mesh, in_specs=in_specs, out_specs=out_specs, check_vma=False)
```

```python
import functools, math
import jax, jax.numpy as jnp, numpy as np
from jax import lax
from jax.experimental import pallas as pl
from jax.experimental.pallas import tpu as pltpu

NORM_EPS = 1e-5
ROPE_THETA = 10000.0
GRP = 8
KSTEP = 768
EARLY = 2


def attend_kernel(sp_size, tok_ref, pos_ref, freq_ref, gain_ref, wq_hbm, wk_hbm, wv_hbm, ck_hbm, cv_hbm,
                  part_ref, nk_hbm, nv_hbm,
                  wq, wk, wv, kbuf, vbuf, acc, normed, qrows, knew, vnew, posrow, wsem, csem, osem):
    rows, width = tok_ref.shape
    slots_local = kbuf.shape[1]
    kv_heads = kbuf.shape[2]
    head = kbuf.shape[3]
    q_cols, k_cols = wq.shape[1], wk.shape[1]
    heads = q_cols // head
    half = head // 2
    slots = slots_local * sp_size
    my_first = lax.axis_index("sp") * slots_local
    groups = rows // GRP
    ksteps = width // KSTEP

    def wcopies(c):
        sl = pl.ds(pl.multiple_of(c * KSTEP, KSTEP), KSTEP)
        return [pltpu.make_async_copy(src.at[sl], dst.at[sl], wsem.at[i, c])
                for i, (src, dst) in enumerate(((wq_hbm, wq), (wk_hbm, wk), (wv_hbm, wv)))]

    def ccopies(g):
        sl = pl.ds(g * GRP, GRP)
        return [pltpu.make_async_copy(ck_hbm.at[sl], kbuf.at[sl], csem.at[0, g]),
                pltpu.make_async_copy(cv_hbm.at[sl], vbuf.at[sl], csem.at[1, g])]

    def ocopies(g):
        sl = pl.ds(g * GRP, GRP)
        return [pltpu.make_async_copy(kbuf.at[sl], nk_hbm.at[sl], osem.at[0, g]),
                pltpu.make_async_copy(vbuf.at[sl], nv_hbm.at[sl], osem.at[1, g])]

    for c in range(ksteps):
        for cp in wcopies(c):
            cp.start()
    wide = tok_ref[...].astype(jnp.float32)
    inv = lax.rsqrt(jnp.mean(wide * wide, axis=-1, keepdims=True) + NORM_EPS)
    normed[...] = (wide * inv * gain_ref[...].astype(jnp.float32).reshape(1, width)).astype(jnp.bfloat16)
    for b in range(rows):
        posrow[b:b + 1, :] = jnp.full((1, half), pos_ref[b], jnp.int32)
    angles = posrow[...].astype(jnp.float32) * freq_ref[...]
    cos, sin = jnp.cos(angles), jnp.sin(angles)
    acc[...] = jnp.zeros_like(acc)

    @pl.loop(0, ksteps)
    def _(c):
        for cp in wcopies(c):
            cp.wait()

        for at, these in ((ksteps - 2, range(EARLY)), (ksteps - 1, range(EARLY, groups))):
            @pl.when(c == at)
            def _():
                for g in these:
                    for cp in ccopies(g):
                        cp.start()

        sl = pl.ds(pl.multiple_of(c * KSTEP, KSTEP), KSTEP)
        lhs = normed[:, sl]
        for w, off, cols in ((wq, 0, q_cols), (wk, q_cols, k_cols), (wv, q_cols + k_cols, k_cols)):
            acc[:, off:off + cols] += jnp.dot(lhs, w[sl, :], preferred_element_type=jnp.float32)

    def rope(off):
        a = acc[:, off:off + half]
        b = acc[:, off + half:off + head]
        return jnp.concatenate([a * cos - b * sin, b * cos + a * sin], axis=-1)

    for h in range(heads):
        q = rope(h * head).astype(jnp.bfloat16).astype(jnp.float32)
        qrows[0, pl.ds(h, rows, stride=heads), :] = q[:, :half]
        qrows[1, pl.ds(h, rows, stride=heads), :] = q[:, half:]
    for h in range(kv_heads):
        knew[:, h, :] = rope(q_cols + h * head)
        off = q_cols + k_cols + h * head
        vnew[:, h, :] = acc[:, off:off + head]

    pair = 8 // heads
    merged = slots_local * kv_heads
    lane = lax.broadcasted_iota(jnp.int32, (8, merged), 1)
    row = lax.broadcasted_iota(jnp.int32, (8, merged), 0)
    lane_slot = my_first + lane // kv_heads
    same_head = (lane % kv_heads) == ((row % heads) // (heads // kv_heads))
    scale = 1.0 / math.sqrt(head)
    stat_lane = lax.broadcasted_iota(jnp.int32, (8, 128), 1)
    n_pairs = GRP // pair
    span = 128 // (2 * n_pairs)

    @pl.loop(0, groups)
    def _(g):
        for cp in ccopies(g):
            cp.wait()
        for i in range(GRP):
            b = g * GRP + i
            local = pos_ref[b] % slots - my_first

            @pl.when((local >= 0) & (local < slots_local))
            def _():
                kbuf[b, local] = knew[b].astype(jnp.bfloat16)
                vbuf[b, local] = vnew[b].astype(jnp.bfloat16)
        for cp in ocopies(g):
            cp.start()
        stat = jnp.zeros((8, 128), jnp.float32)
        for j in range(n_pairs):
            b0 = g * GRP + j * pair
            q_at = pl.ds(pl.multiple_of(b0 * heads, 8), 8)
            q8 = jnp.concatenate([qrows[0, q_at, :], qrows[1, q_at, :]], axis=-1).astype(jnp.bfloat16)
            s = None
            lim = None
            for i in range(pair):
                kk = kbuf[b0 + i].reshape(merged, head)
                si = lax.dot_general(q8, kk, (((1,), (1,)), ((), ())), preferred_element_type=jnp.float32)
                li = jnp.minimum(pos_ref[b0 + i], slots - 1)
                s = si if s is None else jnp.where(row < i * heads, s, si)
                lim = jnp.full((8, merged), li, jnp.int32) if lim is None else jnp.where(row < i * heads, lim, li)
            valid = same_head & (lane_slot <= lim)
            s = jnp.where(valid, s * scale, -jnp.inf)
            top = jnp.max(s, axis=-1, keepdims=True)
            safe = jnp.where(top == -jnp.inf, 0.0, top)
            p = jnp.exp(s - safe)
            total = jnp.sum(p, axis=-1, keepdims=True)
            out = None
            for i in range(pair):
                vv = vbuf[b0 + i].reshape(merged, head)
                mine = (row >= i * heads) & (row < (i + 1) * heads)
                oi = jnp.dot(jnp.where(mine, p, 0.0).astype(jnp.bfloat16), vv, preferred_element_type=jnp.float32)
                out = oi if out is None else out + oi
            part_ref[g, j * 8:(j + 1) * 8, :] = out
            lo = 2 * j * span
            stat = jnp.where((stat_lane >= lo) & (stat_lane < lo + span), top, stat)
            stat = jnp.where((stat_lane >= lo + span) & (stat_lane < lo + 2 * span), total, stat)
        part_ref[g, n_pairs * 8:, :128] = stat
        part_ref[g, n_pairs * 8:, 128:] = stat

    for g in range(groups):
        for cp in ocopies(g):
            cp.wait()


def attend(sp_size, tokens, positions, cache_k, cache_v, gain, w_q, w_k, w_v):
    rows, width = tokens.shape
    _, slots_local, kv_heads, head = cache_k.shape
    heads = w_q.shape[1] // head
    freq = jnp.asarray((np.float32(ROPE_THETA) ** (np.float32(-2.0) * np.arange(head // 2, dtype=np.float32) / np.float32(head))).astype(np.float32))[None, :]
    groups = rows // GRP
    chunk_rows = GRP * heads + 8
    any_spec = pl.BlockSpec(memory_space=pl.ANY)
    vm = pl.BlockSpec(memory_space=pltpu.VMEM)
    qkv_cols = w_q.shape[1] + 2 * w_k.shape[1]
    bf = jnp.bfloat16
    return pl.pallas_call(
        functools.partial(attend_kernel, sp_size),
        out_shape=(jax.ShapeDtypeStruct((groups, chunk_rows, head), jnp.float32),
                   jax.ShapeDtypeStruct(cache_k.shape, bf), jax.ShapeDtypeStruct(cache_v.shape, bf)),
        in_specs=[vm, pl.BlockSpec(memory_space=pltpu.SMEM), vm, vm] + [any_spec] * 5,
        out_specs=(vm, any_spec, any_spec),
        scratch_shapes=[
            pltpu.VMEM(w_q.shape, bf), pltpu.VMEM(w_k.shape, bf), pltpu.VMEM(w_v.shape, bf),
            pltpu.VMEM(cache_k.shape, bf), pltpu.VMEM(cache_v.shape, bf),
            pltpu.VMEM((rows, qkv_cols), jnp.float32), pltpu.VMEM((rows, width), bf),
            pltpu.VMEM((2, rows * heads, head // 2), jnp.float32),
            pltpu.VMEM((rows, kv_heads, head), jnp.float32), pltpu.VMEM((rows, kv_heads, head), jnp.float32),
            pltpu.VMEM((rows, head // 2), jnp.int32),
            pltpu.SemaphoreType.DMA((3, width // KSTEP)), pltpu.SemaphoreType.DMA((2, groups)), pltpu.SemaphoreType.DMA((2, groups)),
        ],
        compiler_params=pltpu.CompilerParams(vmem_limit_bytes=56 << 20),
        name="attend",
    )(tokens, positions, freq, gain, w_q, w_k, w_v, cache_k, cache_v)


MESH_ID = pl.DeviceIdType.MESH
CHUNK = 1024
CORES = 2


def finish_kernel(sp_size, tp_size, part_ref, tok_ref, gain_ref, wo_hbm, wg_hbm, wu_hbm, wd_hbm, out_ref,
                  wo, wg, wu, wd, crecv, att, toks, dsend, drecv, hbuf, normed, hidden_mlp, dpart, precv, gsum, grecv, obuf,
                  wsem, csem, dsem, hsem, qsem, gsem, asem, bsem, psem):
    f32, bf = jnp.float32, jnp.bfloat16
    rows, width = tok_ref.shape
    n_x = sp_size // CORES
    heads_cols = wo.shape[0]
    mlp_cols = wg.shape[1]
    sp, tp = lax.axis_index("sp"), lax.axis_index("tp")
    x, core = sp // CORES, sp % CORES
    flip = 1 - core
    group = rows // sp_size

    def rc(src, dst, ssem, rsem, to_sp, to_tp):
        return pltpu.make_async_remote_copy(src_ref=src, dst_ref=dst, send_sem=ssem, recv_sem=rsem,
                                            device_id={"sp": to_sp, "tp": to_tp}, device_id_type=MESH_ID)

    cols = pl.ds(pl.multiple_of(core * mlp_cols, 128), mlp_cols)
    loads = [pltpu.make_async_copy(wo_hbm, wo.at[:, pl.ds(0, width)], wsem.at[0]),
             pltpu.make_async_copy(wg_hbm.at[:, cols], wg, wsem.at[1]),
             pltpu.make_async_copy(wu_hbm.at[:, cols], wu, wsem.at[2]),
             pltpu.make_async_copy(wd_hbm.at[cols, :], wd.at[:, pl.ds(0, width)], wsem.at[3])]
    loads[0].start()
    pending = []

    def send(copy, *args):
        copy(*args).start()
        pending.append(lambda: copy(*args).wait_send())

    barrier = pltpu.get_barrier_semaphore()
    for k in range(1, sp_size):
        pl.semaphore_signal(barrier, inc=1, device_id={"sp": (sp + k) % sp_size, "tp": tp}, device_id_type=MESH_ID)
    for k in range(1, tp_size):
        pl.semaphore_signal(barrier, inc=1, device_id={"sp": sp, "tp": (tp + k) % tp_size}, device_id_type=MESH_ID)
    pl.semaphore_wait(barrier, sp_size + tp_size - 2)

    def part_copy(k):
        to = (sp + k) % sp_size
        return rc(part_ref.at[to], crecv.at[sp], csem.at[0, k - 1], csem.at[1, k - 1], to, tp)

    for k in range(1, sp_size):
        send(part_copy, k)
    pad = CHUNK * tp_size - width
    wo[:, width:] = jnp.zeros((heads_cols, pad), bf)
    wd[:, width:] = jnp.zeros((mlp_cols, pad), bf)
    for t in range(tp_size):
        w = min(CHUNK, width - t * CHUNK)
        toks[:, t, :, :w] = tok_ref[:, t * CHUNK:t * CHUNK + w].astype(f32).reshape(sp_size, group, w)
        if w < CHUNK:
            toks[:, t, :, w:] = jnp.zeros((sp_size, group, CHUNK - w), f32)
    loads[1].start()
    loads[2].start()
    crecv[sp] = part_ref[sp]
    for k in range(1, sp_size):
        src = (sp + sp_size - k) % sp_size
        rc(crecv.at[src], crecv.at[src], csem.at[0, k - 1], csem.at[1, k - 1], sp, tp).wait_recv()

    loads[3].start()
    n_rows = part_ref.shape[1] - 8
    n_pairs = n_rows // 8
    span = 128 // (2 * n_pairs)
    head = part_ref.shape[2]
    heads = heads_cols // head
    stats = [crecv[i, n_rows:, :128] for i in range(sp_size)]
    top = functools.reduce(jnp.maximum, stats)
    factors = [jnp.exp(st - top) for st in stats]
    for j in range(n_pairs):
        lo = 2 * j * span
        num, den = None, None
        for i in range(sp_size):
            f = factors[i][:, lo:lo + 1]
            o = crecv[i, j * 8:(j + 1) * 8, :] * f
            l = stats[i][:, lo + span:lo + span + 1] * f
            num, den = (o, l) if num is None else (num + o, den + l)
        o = num / den
        att[0, j * 8:(j + 1) * 8, :] = o[:, :head // 2]
        att[1, j * 8:(j + 1) * 8, :] = o[:, head // 2:]
    attended = jnp.concatenate([att[half, pl.ds(h, group, stride=heads), :] for h in range(heads) for half in range(2)], axis=-1).astype(bf)

    loads[0].wait()

    def proj_copy(k):
        to = (tp + k) % tp_size
        return rc(dsend.at[to], drecv.at[k - 1], dsem.at[0, k - 1], dsem.at[1, k - 1], sp, to)

    order = (1, 3, 2) if tp_size == 4 else tuple(range(1, tp_size))
    for k in order + (0,):
        t = (tp + k) % tp_size
        dsend[t] = jnp.dot(attended, wo[:, pl.ds(pl.multiple_of(t * CHUNK, CHUNK), CHUNK)], preferred_element_type=f32)
        if k:
            send(proj_copy, k)
    total = toks[sp, tp] + dsend[tp]
    mine = dsend[tp]
    for k in order:
        rc(drecv.at[k - 1], drecv.at[k - 1], dsem.at[0, k - 1], dsem.at[1, k - 1], sp, tp).wait_recv()
        mine = mine + drecv[k - 1]
    hbuf[core, tp] = (toks[sp, tp] + mine).astype(bf).astype(f32)

    partner = sp + 1 - 2 * core

    def h_copy(k):
        return rc(hbuf.at[core, tp], hbuf.at[core, tp], hsem.at[0, k - 1], hsem.at[1, k - 1], sp, (tp + k) % tp_size)

    def q_copy(k):
        t = (tp + tp_size - k) % tp_size
        return rc(hbuf.at[core, t], hbuf.at[core, t], qsem.at[0, k], qsem.at[1, k], partner, tp)

    for k in order:
        send(h_copy, k)
    send(q_copy, 0)
    for k in order:
        t = (tp + tp_size - k) % tp_size
        rc(hbuf.at[core, t], hbuf.at[core, t], hsem.at[0, k - 1], hsem.at[1, k - 1], sp, tp).wait_recv()
        send(q_copy, k)
    for k in (0,) + order:
        t = (tp + tp_size - k) % tp_size
        rc(hbuf.at[flip, t], hbuf.at[flip, t], qsem.at[0, k], qsem.at[1, k], sp, tp).wait_recv()

    chip_rows = CORES * group
    square = None
    for t in range(tp_size):
        w = min(CHUNK, width - t * CHUNK)
        v = hbuf[:, t].reshape(chip_rows, CHUNK)[:, :w]
        s = jnp.sum(v * v, axis=-1, keepdims=True)
        square = s if square is None else square + s
    inv = lax.rsqrt(square / width + NORM_EPS)
    for t in range(tp_size):
        w = min(CHUNK, width - t * CHUNK)
        v = hbuf[:, t].reshape(chip_rows, CHUNK)[:, :w]
        normed[:, t * CHUNK:t * CHUNK + w] = (v * inv * gain_ref[t * CHUNK:t * CHUNK + w].astype(f32).reshape(1, w)).astype(bf)
    loads[1].wait()
    gate = jnp.dot(normed[...], wg[...], preferred_element_type=f32)
    loads[2].wait()
    up = jnp.dot(normed[...], wu[...], preferred_element_type=f32)
    hidden_mlp[...] = (jax.nn.silu(gate) * up).astype(bf)
    loads[3].wait()

    def half_copy(i):
        t = (tp + i) % tp_size
        return rc(dpart.at[flip, t], precv.at[i], qsem.at[0, tp_size + i], qsem.at[1, tp_size + i], partner, tp)

    def sum_copy(k):
        return rc(gsum.at[k], grecv.at[k - 1], gsem.at[0, k - 1], gsem.at[1, k - 1], sp, (tp + k) % tp_size)

    def pair_sum(i):
        t = (tp + i) % tp_size
        rc(precv.at[i], precv.at[i], qsem.at[0, tp_size + i], qsem.at[1, tp_size + i], sp, tp).wait_recv()
        gsum[i] = dpart[core, t] + precv[i]
        if i:
            send(sum_copy, i)

    steps = order + (0,)
    for n, i in enumerate(steps):
        t = (tp + i) % tp_size
        part = jnp.dot(hidden_mlp[...], wd[:, pl.ds(pl.multiple_of(t * CHUNK, CHUNK), CHUNK)], preferred_element_type=f32)
        dpart[:, t] = part.reshape(CORES, group, CHUNK)
        send(half_copy, i)
        if n >= 2:
            pair_sum(steps[n - 2])
    pair_sum(steps[-2])
    pair_sum(steps[-1])
    acc = gsum[0]
    for k in order:
        rc(grecv.at[k - 1], grecv.at[k - 1], gsem.at[0, k - 1], gsem.at[1, k - 1], sp, tp).wait_recv()
        acc = acc + grecv[k - 1]
    obuf[sp, tp] = (hbuf[core, tp] + acc).astype(bf).astype(f32)

    def gather(buf):
        def chunk(s, t):
            return buf.at[s, t]

        def own_chunk(d_sp, d_tp, c, k, j):
            s = (d_sp + sp_size - CORES * (k * (1 - c) + j * c)) % sp_size
            t = (d_tp + tp_size - (k * c + j * (1 - c))) % tp_size
            return s, t

        def first_copy(k):
            return rc(chunk(sp, tp), chunk(sp, tp), asem.at[0, k - 1], asem.at[1, k - 1],
                      (sp + CORES * k * core) % sp_size, (tp + k * flip) % tp_size)

        def second_copy(k, j):
            s, t = own_chunk(sp, tp, core, 0, j)
            return rc(chunk(s, t), chunk(s, t), bsem.at[0, k - 1, j], bsem.at[1, k - 1, j],
                      (sp + CORES * k * flip) % sp_size, (tp + k * core) % tp_size)

        def pair_copy(k, j):
            s, t = own_chunk(sp, tp, core, k, j)
            return rc(chunk(s, t), chunk(s, t), psem.at[0, k, j], psem.at[1, k, j], partner, tp)

        for k in order:
            send(first_copy, k)
        for k in order:
            send(second_copy, k, 0)
        send(pair_copy, 0, 0)
        for j in order:
            s, t = own_chunk(sp, tp, core, 0, j)
            rc(chunk(s, t), chunk(s, t), asem.at[0, j - 1], asem.at[1, j - 1], sp, tp).wait_recv()
            for k in order:
                send(second_copy, k, j)
            send(pair_copy, 0, j)
        for j in (0,) + order:
            for k in order:
                s, t = own_chunk(sp, tp, core, k, j)
                rc(chunk(s, t), chunk(s, t), bsem.at[0, k - 1, j], bsem.at[1, k - 1, j], sp, tp).wait_recv()
                send(pair_copy, k, j)
        for j in (0,) + order:
            for k in (0,) + order:
                s, t = own_chunk(partner, tp, flip, k, j)
                rc(chunk(s, t), chunk(s, t), psem.at[0, k, j], psem.at[1, k, j], sp, tp).wait_recv()

    gather(obuf)

    for t in range(tp_size):
        w = min(CHUNK, width - t * CHUNK)
        out_ref[:, t * CHUNK:t * CHUNK + w] = obuf[:, t].reshape(rows, CHUNK)[:, :w].astype(bf)
    for done in pending:
        done()


def finish(sp_size, tp_size, part, tokens, gain, w_o, w_gate, w_up, w_down):
    rows, width = tokens.shape
    group = rows // sp_size
    n_x = sp_size // CORES
    mlp_cols = w_gate.shape[1] // CORES
    padded = CHUNK * tp_size
    f32, bf = jnp.float32, jnp.bfloat16
    any_spec = pl.BlockSpec(memory_space=pl.ANY)
    vm = pl.BlockSpec(memory_space=pltpu.VMEM)
    dma = pltpu.SemaphoreType.DMA
    head = part.shape[2]
    return pl.pallas_call(
        functools.partial(finish_kernel, sp_size, tp_size),
        out_shape=jax.ShapeDtypeStruct((rows, width), bf),
        in_specs=[vm, vm, vm] + [any_spec] * 4,
        out_specs=vm,
        scratch_shapes=[
            pltpu.VMEM((w_o.shape[0], padded), bf), pltpu.VMEM((width, mlp_cols), bf), pltpu.VMEM((width, mlp_cols), bf), pltpu.VMEM((mlp_cols, padded), bf),
            pltpu.VMEM(part.shape, f32), pltpu.VMEM((2, part.shape[1] - 8, head // 2), f32),
            pltpu.VMEM((sp_size, tp_size, group, CHUNK), f32),
            pltpu.VMEM((tp_size, group, CHUNK), f32), pltpu.VMEM((tp_size - 1, group, CHUNK), f32),
            pltpu.VMEM((CORES, tp_size, group, CHUNK), f32),
            pltpu.VMEM((CORES * group, width), bf), pltpu.VMEM((CORES * group, mlp_cols), bf),
            pltpu.VMEM((CORES, tp_size, group, CHUNK), f32), pltpu.VMEM((tp_size, group, CHUNK), f32), pltpu.VMEM((tp_size, group, CHUNK), f32),
            pltpu.VMEM((tp_size - 1, group, CHUNK), f32),
            pltpu.VMEM((sp_size, tp_size, group, CHUNK), f32),
            dma((4,)), dma((2, sp_size - 1)), dma((2, tp_size - 1)), dma((2, tp_size - 1)), dma((2, 2 * tp_size)), dma((2, tp_size - 1)),
            dma((2, 3)), dma((2, 3, tp_size)), dma((2, n_x, tp_size)),
        ],
        compiler_params=pltpu.CompilerParams(vmem_limit_bytes=62 << 20, collective_id=0, has_side_effects=True),
        name="finish",
    )(part, tokens, gain, w_o, w_gate, w_up, w_down)


from jax.sharding import PartitionSpec as P


def solution(mesh):
    sp_size, tp_size = mesh.shape["sp"], mesh.shape["tp"]
    cache_spec = P("dp", "sp", "tp", None)
    row_spec = P("dp", None)
    col_spec = P(None, "tp")
    in_specs = (row_spec, P("dp"), cache_spec, cache_spec, P(None), col_spec, col_spec, col_spec, P("tp", None), P(None), col_spec, col_spec, P("tp", None))
    out_specs = (row_spec, cache_spec, cache_spec)

    def local_step(tokens, positions, cache_k, cache_v, attn_gain, w_q, w_k, w_v, w_o, mlp_gain, w_gate, w_up, w_down):
        part, new_k, new_v = attend(sp_size, tokens, positions, cache_k, cache_v, attn_gain, w_q, w_k, w_v)
        layer_out = finish(sp_size, tp_size, part, tokens, mlp_gain, w_o, w_gate, w_up, w_down)
        return layer_out, new_k, new_v

    return jax.shard_map(local_step, mesh=mesh, in_specs=in_specs, out_specs=out_specs, check_vma=False)
```

```python
import functools, math
import jax, jax.numpy as jnp, numpy as np
from jax import lax
from jax.experimental import pallas as pl
from jax.experimental.pallas import tpu as pltpu

NORM_EPS = 1e-5
ROPE_THETA = 10000.0
GRP = 8
KSTEP = 768
AHEAD = 3


def attend_kernel(sp_size, tok_hbm, pos_hbm, freq_hbm, gain_hbm, wq_hbm, wk_hbm, wv_hbm, ck_hbm, cv_hbm,
                  part_ref, nk_hbm, nv_hbm,
                  tok_ref, pos_ref, freq_ref, gain_ref, wq, wk, wv, kbuf, vbuf, acc, normed, qrows, knew, vnew, posrow, isem, wsem, csem, osem):
    rows, width = tok_ref.shape
    slots_local = kbuf.shape[1]
    kv_heads = kbuf.shape[2]
    head = kbuf.shape[3]
    q_cols, k_cols = wq.shape[1], wk.shape[1]
    heads = q_cols // head
    half = head // 2
    slots = slots_local * sp_size
    my_first = lax.axis_index("sp") * slots_local
    groups = rows // GRP
    ksteps = width // KSTEP

    def wcopies(c):
        sl = pl.ds(pl.multiple_of(c * KSTEP, KSTEP), KSTEP)
        return [pltpu.make_async_copy(src.at[sl], dst.at[sl], wsem.at[i, c])
                for i, (src, dst) in enumerate(((wq_hbm, wq), (wk_hbm, wk), (wv_hbm, wv)))]

    def ccopies(g):
        sl = pl.ds(g * GRP, GRP)
        return [pltpu.make_async_copy(ck_hbm.at[sl], kbuf.at[sl], csem.at[0, g]),
                pltpu.make_async_copy(cv_hbm.at[sl], vbuf.at[sl], csem.at[1, g])]

    def ocopies(g):
        sl = pl.ds(g * GRP, GRP)
        return [pltpu.make_async_copy(kbuf.at[sl], nk_hbm.at[sl], osem.at[0, g]),
                pltpu.make_async_copy(vbuf.at[sl], nv_hbm.at[sl], osem.at[1, g])]

    inputs = [pltpu.make_async_copy(src, dst, isem.at[i])
              for i, (src, dst) in enumerate(((tok_hbm, tok_ref), (pos_hbm, pos_ref), (freq_hbm, freq_ref), (gain_hbm, gain_ref)))]
    for cp in inputs:
        cp.start()
    for c in range(AHEAD):
        for cp in wcopies(c):
            cp.start()
    for cp in inputs:
        cp.wait()
    wide = tok_ref[...].astype(jnp.float32)
    inv = lax.rsqrt(jnp.mean(wide * wide, axis=-1, keepdims=True) + NORM_EPS)
    normed[...] = (wide * inv * gain_ref[...].astype(jnp.float32).reshape(1, width)).astype(jnp.bfloat16)
    for b in range(rows):
        posrow[b:b + 1, :] = jnp.full((1, half), pos_ref[b], jnp.int32)
    angles = posrow[...].astype(jnp.float32) * freq_ref[...]
    cos, sin = jnp.cos(angles), jnp.sin(angles)
    acc[...] = jnp.zeros_like(acc)

    @pl.loop(0, ksteps)
    def _(c):
        for cp in wcopies(c):
            cp.wait()

        @pl.when(c + AHEAD < ksteps)
        def _():
            for cp in wcopies(c + AHEAD):
                cp.start()

        @pl.when(c + AHEAD >= ksteps)
        def _():
            for cp in ccopies(c + AHEAD - ksteps):
                cp.start()

        sl = pl.ds(pl.multiple_of(c * KSTEP, KSTEP), KSTEP)
        lhs = normed[:, sl]
        for w, off, cols in ((wq, 0, q_cols), (wk, q_cols, k_cols), (wv, q_cols + k_cols, k_cols)):
            acc[:, off:off + cols] += jnp.dot(lhs, w[sl, :], preferred_element_type=jnp.float32)

    def rope(off):
        a = acc[:, off:off + half]
        b = acc[:, off + half:off + head]
        return jnp.concatenate([a * cos - b * sin, b * cos + a * sin], axis=-1)

    for h in range(heads):
        q = rope(h * head).astype(jnp.bfloat16).astype(jnp.float32)
        qrows[0, pl.ds(h, rows, stride=heads), :] = q[:, :half]
        qrows[1, pl.ds(h, rows, stride=heads), :] = q[:, half:]
    for h in range(kv_heads):
        knew[:, h, :] = rope(q_cols + h * head)
        off = q_cols + k_cols + h * head
        vnew[:, h, :] = acc[:, off:off + head]

    pair = 8 // heads
    merged = slots_local * kv_heads
    lane = lax.broadcasted_iota(jnp.int32, (8, merged), 1)
    row = lax.broadcasted_iota(jnp.int32, (8, merged), 0)
    lane_slot = my_first + lane // kv_heads
    same_head = (lane % kv_heads) == ((row % heads) // (heads // kv_heads))
    scale = 1.0 / math.sqrt(head)
    stat_lane = lax.broadcasted_iota(jnp.int32, (8, 128), 1)
    n_pairs = GRP // pair
    span = 128 // (2 * n_pairs)

    @pl.loop(0, groups)
    def _(g):
        for cp in ccopies(g):
            cp.wait()

        @pl.when(g + AHEAD < groups)
        def _():
            for cp in ccopies(g + AHEAD):
                cp.start()

        for i in range(GRP):
            b = g * GRP + i
            local = pos_ref[b] % slots - my_first

            @pl.when((local >= 0) & (local < slots_local))
            def _():
                kbuf[b, local] = knew[b].astype(jnp.bfloat16)
                vbuf[b, local] = vnew[b].astype(jnp.bfloat16)
        for cp in ocopies(g):
            cp.start()
        stat = jnp.zeros((8, 128), jnp.float32)
        for j in range(n_pairs):
            b0 = g * GRP + j * pair
            q_at = pl.ds(pl.multiple_of(b0 * heads, 8), 8)
            q8 = jnp.concatenate([qrows[0, q_at, :], qrows[1, q_at, :]], axis=-1).astype(jnp.bfloat16)
            s = None
            lim = None
            for i in range(pair):
                kk = kbuf[b0 + i].reshape(merged, head)
                si = lax.dot_general(q8, kk, (((1,), (1,)), ((), ())), preferred_element_type=jnp.float32)
                li = jnp.minimum(pos_ref[b0 + i], slots - 1)
                s = si if s is None else jnp.where(row < i * heads, s, si)
                lim = jnp.full((8, merged), li, jnp.int32) if lim is None else jnp.where(row < i * heads, lim, li)
            valid = same_head & (lane_slot <= lim)
            s = jnp.where(valid, s * scale, -jnp.inf)
            top = jnp.max(s, axis=-1, keepdims=True)
            safe = jnp.where(top == -jnp.inf, 0.0, top)
            p = jnp.exp(s - safe)
            total = jnp.sum(p, axis=-1, keepdims=True)
            out = None
            for i in range(pair):
                vv = vbuf[b0 + i].reshape(merged, head)
                mine = (row >= i * heads) & (row < (i + 1) * heads)
                oi = jnp.dot(jnp.where(mine, p, 0.0).astype(jnp.bfloat16), vv, preferred_element_type=jnp.float32)
                out = oi if out is None else out + oi
            part_ref[g, j * 8:(j + 1) * 8, :] = out
            lo = 2 * j * span
            stat = jnp.where((stat_lane >= lo) & (stat_lane < lo + span), top, stat)
            stat = jnp.where((stat_lane >= lo + span) & (stat_lane < lo + 2 * span), total, stat)
        part_ref[g, n_pairs * 8:, :128] = stat
        part_ref[g, n_pairs * 8:, 128:] = stat

    for g in range(groups):
        for cp in ocopies(g):
            cp.wait()


def attend(sp_size, tokens, positions, cache_k, cache_v, gain, w_q, w_k, w_v):
    rows, width = tokens.shape
    _, slots_local, kv_heads, head = cache_k.shape
    heads = w_q.shape[1] // head
    freq = jnp.asarray((np.float32(ROPE_THETA) ** (np.float32(-2.0) * np.arange(head // 2, dtype=np.float32) / np.float32(head))).astype(np.float32))[None, :]
    groups = rows // GRP
    chunk_rows = GRP * heads + 8
    any_spec = pl.BlockSpec(memory_space=pltpu.HBM)
    vm = pl.BlockSpec(memory_space=pltpu.VMEM)
    qkv_cols = w_q.shape[1] + 2 * w_k.shape[1]
    bf = jnp.bfloat16
    return pl.pallas_call(
        functools.partial(attend_kernel, sp_size),
        out_shape=(pltpu.VMEM((groups, chunk_rows, head), jnp.float32),
                   jax.ShapeDtypeStruct(cache_k.shape, bf), jax.ShapeDtypeStruct(cache_v.shape, bf)),
        in_specs=[any_spec] * 9,
        out_specs=(vm, any_spec, any_spec),
        scratch_shapes=[
            pltpu.VMEM(tokens.shape, bf), pltpu.SMEM(positions.shape, jnp.int32), pltpu.VMEM((1, head // 2), jnp.float32), pltpu.VMEM(gain.shape, bf),
            pltpu.VMEM(w_q.shape, bf), pltpu.VMEM(w_k.shape, bf), pltpu.VMEM(w_v.shape, bf),
            pltpu.VMEM(cache_k.shape, bf), pltpu.VMEM(cache_v.shape, bf),
            pltpu.VMEM((rows, qkv_cols), jnp.float32), pltpu.VMEM((rows, width), bf),
            pltpu.VMEM((2, rows * heads, head // 2), jnp.float32),
            pltpu.VMEM((rows, kv_heads, head), jnp.float32), pltpu.VMEM((rows, kv_heads, head), jnp.float32),
            pltpu.VMEM((rows, head // 2), jnp.int32),
            pltpu.SemaphoreType.DMA((4,)), pltpu.SemaphoreType.DMA((3, width // KSTEP)), pltpu.SemaphoreType.DMA((2, groups)), pltpu.SemaphoreType.DMA((2, groups)),
        ],
        compiler_params=pltpu.CompilerParams(vmem_limit_bytes=66_000_000),
        name="attend",
    )(tokens, positions, freq, gain, w_q, w_k, w_v, cache_k, cache_v)


MESH_ID = pl.DeviceIdType.MESH
CHUNK = 1024
CORES = 2


def finish_kernel(sp_size, tp_size, part_ref, tok_hbm, gain_hbm, wo_hbm, wg_hbm, wu_hbm, wd_hbm, out_ref,
                  tok_ref, gain_ref, wo, wg, wu, wd, crecv, att, toks, dsend, drecv, hbuf, normed, hidden_mlp, dpart, precv, gsum, grecv, obuf,
                  wsem, csem, dsem, hsem, qsem, gsem, asem, bsem, psem):
    f32, bf = jnp.float32, jnp.bfloat16
    rows, width = tok_ref.shape
    n_x = sp_size // CORES
    heads_cols = wo.shape[0]
    mlp_cols = wg.shape[1]
    sp, tp = lax.axis_index("sp"), lax.axis_index("tp")
    x, core = sp // CORES, sp % CORES
    flip = 1 - core
    group = rows // sp_size

    def rc(src, dst, ssem, rsem, to_sp, to_tp):
        return pltpu.make_async_remote_copy(src_ref=src, dst_ref=dst, send_sem=ssem, recv_sem=rsem,
                                            device_id={"sp": to_sp, "tp": to_tp}, device_id_type=MESH_ID)

    cols = pl.ds(pl.multiple_of(core * mlp_cols, 128), mlp_cols)
    loads = [pltpu.make_async_copy(wo_hbm, wo.at[:, pl.ds(0, width)], wsem.at[0]),
             pltpu.make_async_copy(wg_hbm.at[:, cols], wg, wsem.at[1]),
             pltpu.make_async_copy(wu_hbm.at[:, cols], wu, wsem.at[2]),
             pltpu.make_async_copy(wd_hbm.at[cols, :], wd.at[:, pl.ds(0, width)], wsem.at[3]),
             pltpu.make_async_copy(tok_hbm, tok_ref, wsem.at[4]),
             pltpu.make_async_copy(gain_hbm, gain_ref, wsem.at[5])]
    for cp in (loads[4], loads[5], loads[0]):
        cp.start()
    pending = []

    def send(copy, *args):
        copy(*args).start()
        pending.append(lambda: copy(*args).wait_send())

    barrier = pltpu.get_barrier_semaphore()
    for k in range(1, sp_size):
        pl.semaphore_signal(barrier, inc=1, device_id={"sp": (sp + k) % sp_size, "tp": tp}, device_id_type=MESH_ID)
    for k in range(1, tp_size):
        pl.semaphore_signal(barrier, inc=1, device_id={"sp": sp, "tp": (tp + k) % tp_size}, device_id_type=MESH_ID)
    pl.semaphore_wait(barrier, sp_size + tp_size - 2)

    def part_copy(k):
        to = (sp + k) % sp_size
        return rc(part_ref.at[to], crecv.at[sp], csem.at[0, k - 1], csem.at[1, k - 1], to, tp)

    for k in sorted(range(1, sp_size), key=lambda k: abs(k - sp_size // 2)):
        send(part_copy, k)
    pad = CHUNK * tp_size - width
    wo[:, width:] = jnp.zeros((heads_cols, pad), bf)
    wd[:, width:] = jnp.zeros((mlp_cols, pad), bf)
    loads[4].wait()
    loads[5].wait()
    for t in range(tp_size):
        w = min(CHUNK, width - t * CHUNK)
        toks[:, t, :, :w] = tok_ref[:, t * CHUNK:t * CHUNK + w].astype(f32).reshape(sp_size, group, w)
        if w < CHUNK:
            toks[:, t, :, w:] = jnp.zeros((sp_size, group, CHUNK - w), f32)
    loads[1].start()
    crecv[sp] = part_ref[sp]
    for k in range(1, sp_size):
        src = (sp + sp_size - k) % sp_size
        rc(crecv.at[src], crecv.at[src], csem.at[0, k - 1], csem.at[1, k - 1], sp, tp).wait_recv()

    loads[2].start()
    n_rows = part_ref.shape[1] - 8
    n_pairs = n_rows // 8
    span = 128 // (2 * n_pairs)
    head = part_ref.shape[2]
    heads = heads_cols // head
    stats = [crecv[i, n_rows:, :128] for i in range(sp_size)]
    top = functools.reduce(jnp.maximum, stats)
    factors = [jnp.exp(st - top) for st in stats]
    for j in range(n_pairs):
        lo = 2 * j * span
        num, den = None, None
        for i in range(sp_size):
            f = factors[i][:, lo:lo + 1]
            o = crecv[i, j * 8:(j + 1) * 8, :] * f
            l = stats[i][:, lo + span:lo + span + 1] * f
            num, den = (o, l) if num is None else (num + o, den + l)
        o = num / den
        att[0, j * 8:(j + 1) * 8, :] = o[:, :head // 2]
        att[1, j * 8:(j + 1) * 8, :] = o[:, head // 2:]
    attended = jnp.concatenate([att[half, pl.ds(h, group, stride=heads), :] for h in range(heads) for half in range(2)], axis=-1).astype(bf)

    loads[0].wait()

    def proj_copy(k):
        to = (tp + k) % tp_size
        return rc(dsend.at[to], drecv.at[k - 1], dsem.at[0, k - 1], dsem.at[1, k - 1], sp, to)

    far_first, order = (2, 1, 3), (1, 3, 2)
    for k in far_first + (0,):
        t = (tp + k) % tp_size
        dsend[t] = jnp.dot(attended, wo[:, pl.ds(pl.multiple_of(t * CHUNK, CHUNK), CHUNK)], preferred_element_type=f32)
        if k:
            send(proj_copy, k)
    total = toks[sp, tp] + dsend[tp]
    mine = dsend[tp]
    for k in order:
        rc(drecv.at[k - 1], drecv.at[k - 1], dsem.at[0, k - 1], dsem.at[1, k - 1], sp, tp).wait_recv()
        mine = mine + drecv[k - 1]
    hbuf[core, tp] = (toks[sp, tp] + mine).astype(bf).astype(f32)

    loads[3].start()

    partner = sp + 1 - 2 * core

    def h_copy(k):
        return rc(hbuf.at[core, tp], hbuf.at[core, tp], hsem.at[0, k - 1], hsem.at[1, k - 1], sp, (tp + k) % tp_size)

    def q_copy(k):
        t = (tp + tp_size - k) % tp_size
        return rc(hbuf.at[core, t], hbuf.at[core, t], qsem.at[0, k], qsem.at[1, k], partner, tp)

    for k in far_first:
        send(h_copy, k)
    send(q_copy, 0)
    for k in order:
        t = (tp + tp_size - k) % tp_size
        rc(hbuf.at[core, t], hbuf.at[core, t], hsem.at[0, k - 1], hsem.at[1, k - 1], sp, tp).wait_recv()
        send(q_copy, k)
    for k in (0,) + order:
        t = (tp + tp_size - k) % tp_size
        rc(hbuf.at[flip, t], hbuf.at[flip, t], qsem.at[0, k], qsem.at[1, k], sp, tp).wait_recv()

    chip_rows = CORES * group
    square = None
    for t in range(tp_size):
        w = min(CHUNK, width - t * CHUNK)
        v = hbuf[:, t].reshape(chip_rows, CHUNK)[:, :w]
        s = jnp.sum(v * v, axis=-1, keepdims=True)
        square = s if square is None else square + s
    inv = lax.rsqrt(square / width + NORM_EPS)
    for t in range(tp_size):
        w = min(CHUNK, width - t * CHUNK)
        v = hbuf[:, t].reshape(chip_rows, CHUNK)[:, :w]
        normed[:, t * CHUNK:t * CHUNK + w] = (v * inv * gain_ref[t * CHUNK:t * CHUNK + w].astype(f32).reshape(1, w)).astype(bf)
    loads[1].wait()
    gate = jnp.dot(normed[...], wg[...], preferred_element_type=f32)
    loads[2].wait()
    up = jnp.dot(normed[...], wu[...], preferred_element_type=f32)
    hidden_mlp[...] = (jax.nn.silu(gate) * up).astype(bf)
    loads[3].wait()

    def half_copy(i):
        t = (tp + i) % tp_size
        return rc(dpart.at[flip, t], precv.at[i], qsem.at[0, tp_size + i], qsem.at[1, tp_size + i], partner, tp)

    def sum_copy(k):
        return rc(gsum.at[k], grecv.at[k - 1], gsem.at[0, k - 1], gsem.at[1, k - 1], sp, (tp + k) % tp_size)

    def pair_sum(i):
        t = (tp + i) % tp_size
        rc(precv.at[i], precv.at[i], qsem.at[0, tp_size + i], qsem.at[1, tp_size + i], sp, tp).wait_recv()
        gsum[i] = dpart[core, t] + precv[i]
        if i:
            send(sum_copy, i)

    steps = far_first + (0,)
    for n, i in enumerate(steps):
        t = (tp + i) % tp_size
        part = jnp.dot(hidden_mlp[...], wd[:, pl.ds(pl.multiple_of(t * CHUNK, CHUNK), CHUNK)], preferred_element_type=f32)
        dpart[:, t] = part.reshape(CORES, group, CHUNK)
        send(half_copy, i)
        if n >= 2:
            pair_sum(steps[n - 2])
    pair_sum(steps[-2])
    pair_sum(steps[-1])
    acc = gsum[0]
    for k in order:
        rc(grecv.at[k - 1], grecv.at[k - 1], gsem.at[0, k - 1], gsem.at[1, k - 1], sp, tp).wait_recv()
        acc = acc + grecv[k - 1]
    obuf[sp, tp] = (hbuf[core, tp] + acc).astype(bf).astype(f32)

    def gather(buf):
        def chunk(s, t):
            return buf.at[s, t]

        def own_chunk(d_sp, d_tp, c, k, j):
            s = (d_sp + sp_size - CORES * (k * (1 - c) + j * c)) % sp_size
            t = (d_tp + tp_size - (k * c + j * (1 - c))) % tp_size
            return s, t

        def first_copy(k):
            return rc(chunk(sp, tp), chunk(sp, tp), asem.at[0, k - 1], asem.at[1, k - 1],
                      (sp + CORES * k * core) % sp_size, (tp + k * flip) % tp_size)

        def second_copy(k, j):
            s, t = own_chunk(sp, tp, core, 0, j)
            return rc(chunk(s, t), chunk(s, t), bsem.at[0, k - 1, j], bsem.at[1, k - 1, j],
                      (sp + CORES * k * flip) % sp_size, (tp + k * core) % tp_size)

        def pair_copy(k, j):
            s, t = own_chunk(sp, tp, core, k, j)
            return rc(chunk(s, t), chunk(s, t), psem.at[0, k, j], psem.at[1, k, j], partner, tp)

        for k in far_first:
            send(first_copy, k)
        for k in far_first:
            send(second_copy, k, 0)
        send(pair_copy, 0, 0)
        for j in order:
            s, t = own_chunk(sp, tp, core, 0, j)
            rc(chunk(s, t), chunk(s, t), asem.at[0, j - 1], asem.at[1, j - 1], sp, tp).wait_recv()
            for k in far_first:
                send(second_copy, k, j)
            send(pair_copy, 0, j)
        for j in (0,) + order:
            for k in order:
                s, t = own_chunk(sp, tp, core, k, j)
                rc(chunk(s, t), chunk(s, t), bsem.at[0, k - 1, j], bsem.at[1, k - 1, j], sp, tp).wait_recv()
                send(pair_copy, k, j)
        for j in (0,) + order:
            for k in (0,) + order:
                s, t = own_chunk(partner, tp, flip, k, j)
                rc(chunk(s, t), chunk(s, t), psem.at[0, k, j], psem.at[1, k, j], sp, tp).wait_recv()

    gather(obuf)

    for t in range(tp_size):
        w = min(CHUNK, width - t * CHUNK)
        out_ref[:, t * CHUNK:t * CHUNK + w] = obuf[:, t].reshape(rows, CHUNK)[:, :w].astype(bf)
    for done in pending:
        done()


def finish(sp_size, tp_size, part, tokens, gain, w_o, w_gate, w_up, w_down):
    rows, width = tokens.shape
    group = rows // sp_size
    n_x = sp_size // CORES
    mlp_cols = w_gate.shape[1] // CORES
    padded = CHUNK * tp_size
    f32, bf = jnp.float32, jnp.bfloat16
    any_spec = pl.BlockSpec(memory_space=pltpu.HBM)
    vm = pl.BlockSpec(memory_space=pltpu.VMEM)
    dma = pltpu.SemaphoreType.DMA
    head = part.shape[2]
    return pl.pallas_call(
        functools.partial(finish_kernel, sp_size, tp_size),
        out_shape=pltpu.VMEM((rows, width), bf),
        in_specs=[vm] + [any_spec] * 6,
        out_specs=vm,
        scratch_shapes=[
            pltpu.VMEM(tokens.shape, bf), pltpu.VMEM(gain.shape, bf),
            pltpu.VMEM((w_o.shape[0], padded), bf), pltpu.VMEM((width, mlp_cols), bf), pltpu.VMEM((width, mlp_cols), bf), pltpu.VMEM((mlp_cols, padded), bf),
            pltpu.VMEM(part.shape, f32), pltpu.VMEM((2, part.shape[1] - 8, head // 2), f32),
            pltpu.VMEM((sp_size, tp_size, group, CHUNK), f32),
            pltpu.VMEM((tp_size, group, CHUNK), f32), pltpu.VMEM((tp_size - 1, group, CHUNK), f32),
            pltpu.VMEM((CORES, tp_size, group, CHUNK), f32),
            pltpu.VMEM((CORES * group, width), bf), pltpu.VMEM((CORES * group, mlp_cols), bf),
            pltpu.VMEM((CORES, tp_size, group, CHUNK), f32), pltpu.VMEM((tp_size, group, CHUNK), f32), pltpu.VMEM((tp_size, group, CHUNK), f32),
            pltpu.VMEM((tp_size - 1, group, CHUNK), f32),
            pltpu.VMEM((sp_size, tp_size, group, CHUNK), f32),
            dma((6,)), dma((2, sp_size - 1)), dma((2, tp_size - 1)), dma((2, tp_size - 1)), dma((2, 2 * tp_size)), dma((2, tp_size - 1)),
            dma((2, 3)), dma((2, 3, tp_size)), dma((2, n_x, tp_size)),
        ],
        compiler_params=pltpu.CompilerParams(vmem_limit_bytes=65_500_000, collective_id=0, has_side_effects=True),
        name="finish",
    )(part, tokens, gain, w_o, w_gate, w_up, w_down)


from jax.sharding import PartitionSpec as P


def solution(mesh):
    sp_size, tp_size = mesh.shape["sp"], mesh.shape["tp"]
    cache_spec = P("dp", "sp", "tp", None)
    row_spec = P("dp", None)
    col_spec = P(None, "tp")
    in_specs = (row_spec, P("dp"), cache_spec, cache_spec, P(None), col_spec, col_spec, col_spec, P("tp", None), P(None), col_spec, col_spec, P("tp", None))
    out_specs = (row_spec, cache_spec, cache_spec)

    def local_step(tokens, positions, cache_k, cache_v, attn_gain, w_q, w_k, w_v, w_o, mlp_gain, w_gate, w_up, w_down):
        part, new_k, new_v = attend(sp_size, tokens, positions, cache_k, cache_v, attn_gain, w_q, w_k, w_v)
        part = pltpu.with_memory_space_constraint(part, pltpu.VMEM)
        layer_out = finish(sp_size, tp_size, part, tokens, mlp_gain, w_o, w_gate, w_up, w_down)
        return layer_out, new_k, new_v

    return jax.shard_map(local_step, mesh=mesh, in_specs=in_specs, out_specs=out_specs, check_vma=False)
```

```python
import functools, math
import jax, jax.numpy as jnp, numpy as np
from jax import lax
from jax.experimental import pallas as pl
from jax.experimental.pallas import tpu as pltpu

NORM_EPS = 1e-5
ROPE_THETA = 10000.0
GRP = 8
KSTEP = 768
AHEAD = 3


def attend_kernel(sp_size, tok_hbm, pos_hbm, freq_hbm, gain_hbm, wq_hbm, wk_hbm, wv_hbm, ck_hbm, cv_hbm,
                  part_ref, nk_hbm, nv_hbm,
                  tok_ref, pos_ref, freq_ref, gain_ref, wq, wk, wv, kbuf, vbuf, acc, normed, qrows, knew, vnew, posrow, isem, wsem, csem, osem):
    rows, width = tok_ref.shape
    slots_local = kbuf.shape[1]
    kv_heads = kbuf.shape[2]
    head = kbuf.shape[3]
    q_cols, k_cols = wq.shape[1], wk.shape[1]
    heads = q_cols // head
    half = head // 2
    slots = slots_local * sp_size
    my_first = lax.axis_index("sp") * slots_local
    groups = rows // GRP
    ksteps = width // KSTEP

    def wcopies(c):
        sl = pl.ds(pl.multiple_of(c * KSTEP, KSTEP), KSTEP)
        return [pltpu.make_async_copy(src.at[sl], dst.at[sl], wsem.at[i, c])
                for i, (src, dst) in enumerate(((wq_hbm, wq), (wk_hbm, wk), (wv_hbm, wv)))]

    def ccopies(g):
        sl = pl.ds(g * GRP, GRP)
        return [pltpu.make_async_copy(ck_hbm.at[sl], kbuf.at[sl], csem.at[0, g]),
                pltpu.make_async_copy(cv_hbm.at[sl], vbuf.at[sl], csem.at[1, g])]

    def ocopies(g):
        sl = pl.ds(g * GRP, GRP)
        return [pltpu.make_async_copy(kbuf.at[sl], nk_hbm.at[sl], osem.at[0, g]),
                pltpu.make_async_copy(vbuf.at[sl], nv_hbm.at[sl], osem.at[1, g])]

    inputs = [pltpu.make_async_copy(src, dst, isem.at[i])
              for i, (src, dst) in enumerate(((tok_hbm, tok_ref), (pos_hbm, pos_ref), (freq_hbm, freq_ref), (gain_hbm, gain_ref)))]
    for cp in inputs:
        cp.start()
    for c in range(AHEAD):
        for cp in wcopies(c):
            cp.start()
    for cp in inputs:
        cp.wait()
    wide = tok_ref[...].astype(jnp.float32)
    inv = lax.rsqrt(jnp.mean(wide * wide, axis=-1, keepdims=True) + NORM_EPS)
    normed[...] = (wide * inv * gain_ref[...].astype(jnp.float32).reshape(1, width)).astype(jnp.bfloat16)
    for b in range(rows):
        posrow[b:b + 1, :] = jnp.full((1, half), pos_ref[b], jnp.int32)
    angles = posrow[...].astype(jnp.float32) * freq_ref[...]
    cos, sin = jnp.cos(angles), jnp.sin(angles)
    acc[...] = jnp.zeros_like(acc)

    @pl.loop(0, ksteps)
    def _(c):
        for cp in wcopies(c):
            cp.wait()

        @pl.when(c + AHEAD < ksteps)
        def _():
            for cp in wcopies(c + AHEAD):
                cp.start()

        @pl.when(c + AHEAD >= ksteps)
        def _():
            for cp in ccopies(c + AHEAD - ksteps):
                cp.start()

        sl = pl.ds(pl.multiple_of(c * KSTEP, KSTEP), KSTEP)
        lhs = normed[:, sl]
        for w, off, cols in ((wq, 0, q_cols), (wk, q_cols, k_cols), (wv, q_cols + k_cols, k_cols)):
            acc[:, off:off + cols] += jnp.dot(lhs, w[sl, :], preferred_element_type=jnp.float32)

    def rope(off):
        a = acc[:, off:off + half]
        b = acc[:, off + half:off + head]
        return jnp.concatenate([a * cos - b * sin, b * cos + a * sin], axis=-1)

    for h in range(heads):
        q = rope(h * head).astype(jnp.bfloat16).astype(jnp.float32)
        qrows[0, pl.ds(h, rows, stride=heads), :] = q[:, :half]
        qrows[1, pl.ds(h, rows, stride=heads), :] = q[:, half:]
    for h in range(kv_heads):
        knew[:, h, :] = rope(q_cols + h * head)
        off = q_cols + k_cols + h * head
        vnew[:, h, :] = acc[:, off:off + head]

    pair = 8 // heads
    merged = slots_local * kv_heads
    lane = lax.broadcasted_iota(jnp.int32, (8, merged), 1)
    row = lax.broadcasted_iota(jnp.int32, (8, merged), 0)
    lane_slot = my_first + lane // kv_heads
    same_head = (lane % kv_heads) == ((row % heads) // (heads // kv_heads))
    scale = 1.0 / math.sqrt(head)
    stat_lane = lax.broadcasted_iota(jnp.int32, (8, 128), 1)
    n_pairs = GRP // pair
    span = 128 // (2 * n_pairs)

    @pl.loop(0, groups)
    def _(g):
        for cp in ccopies(g):
            cp.wait()

        @pl.when(g + AHEAD < groups)
        def _():
            for cp in ccopies(g + AHEAD):
                cp.start()

        for i in range(GRP):
            b = g * GRP + i
            local = pos_ref[b] % slots - my_first
            here = (local >= 0) & (local < slots_local)
            at = jnp.clip(local, 0, slots_local - 1)
            for buf, new in ((kbuf, knew), (vbuf, vnew)):
                buf[b, at] = jnp.where(here, new[b], buf[b, at].astype(jnp.float32)).astype(jnp.bfloat16)
        for cp in ocopies(g):
            cp.start()
        stat = jnp.zeros((8, 128), jnp.float32)
        for j in range(n_pairs):
            b0 = g * GRP + j * pair
            q_at = pl.ds(pl.multiple_of(b0 * heads, 8), 8)
            q8 = jnp.concatenate([qrows[0, q_at, :], qrows[1, q_at, :]], axis=-1).astype(jnp.bfloat16)
            s = None
            lim = None
            for i in range(pair):
                kk = kbuf[b0 + i].reshape(merged, head)
                si = lax.dot_general(q8, kk, (((1,), (1,)), ((), ())), preferred_element_type=jnp.float32)
                li = jnp.minimum(pos_ref[b0 + i], slots - 1)
                s = si if s is None else jnp.where(row < i * heads, s, si)
                lim = jnp.full((8, merged), li, jnp.int32) if lim is None else jnp.where(row < i * heads, lim, li)
            valid = same_head & (lane_slot <= lim)
            s = jnp.where(valid, s * scale, -jnp.inf)
            top = jnp.max(s, axis=-1, keepdims=True)
            safe = jnp.where(top == -jnp.inf, 0.0, top)
            p = jnp.exp(s - safe)
            total = jnp.sum(p, axis=-1, keepdims=True)
            out = None
            for i in range(pair):
                vv = vbuf[b0 + i].reshape(merged, head)
                mine = (row >= i * heads) & (row < (i + 1) * heads)
                oi = jnp.dot(jnp.where(mine, p, 0.0).astype(jnp.bfloat16), vv, preferred_element_type=jnp.float32)
                out = oi if out is None else out + oi
            part_ref[g, j * 8:(j + 1) * 8, :] = out
            lo = 2 * j * span
            stat = jnp.where((stat_lane >= lo) & (stat_lane < lo + span), top, stat)
            stat = jnp.where((stat_lane >= lo + span) & (stat_lane < lo + 2 * span), total, stat)
        part_ref[g, n_pairs * 8:, :128] = stat
        part_ref[g, n_pairs * 8:, 128:] = stat

    for g in range(groups):
        for cp in ocopies(g):
            cp.wait()


def attend(sp_size, tokens, positions, cache_k, cache_v, gain, w_q, w_k, w_v):
    rows, width = tokens.shape
    _, slots_local, kv_heads, head = cache_k.shape
    heads = w_q.shape[1] // head
    freq = jnp.asarray((np.float32(ROPE_THETA) ** (np.float32(-2.0) * np.arange(head // 2, dtype=np.float32) / np.float32(head))).astype(np.float32))[None, :]
    groups = rows // GRP
    chunk_rows = GRP * heads + 8
    any_spec = pl.BlockSpec(memory_space=pltpu.HBM)
    vm = pl.BlockSpec(memory_space=pltpu.VMEM)
    qkv_cols = w_q.shape[1] + 2 * w_k.shape[1]
    bf = jnp.bfloat16
    return pl.pallas_call(
        functools.partial(attend_kernel, sp_size),
        out_shape=(pltpu.VMEM((groups, chunk_rows, head), jnp.float32),
                   jax.ShapeDtypeStruct(cache_k.shape, bf), jax.ShapeDtypeStruct(cache_v.shape, bf)),
        in_specs=[any_spec] * 9,
        out_specs=(vm, any_spec, any_spec),
        scratch_shapes=[
            pltpu.VMEM(tokens.shape, bf), pltpu.SMEM(positions.shape, jnp.int32), pltpu.VMEM((1, head // 2), jnp.float32), pltpu.VMEM(gain.shape, bf),
            pltpu.VMEM(w_q.shape, bf), pltpu.VMEM(w_k.shape, bf), pltpu.VMEM(w_v.shape, bf),
            pltpu.VMEM(cache_k.shape, bf), pltpu.VMEM(cache_v.shape, bf),
            pltpu.VMEM((rows, qkv_cols), jnp.float32), pltpu.VMEM((rows, width), bf),
            pltpu.VMEM((2, rows * heads, head // 2), jnp.float32),
            pltpu.VMEM((rows, kv_heads, head), jnp.float32), pltpu.VMEM((rows, kv_heads, head), jnp.float32),
            pltpu.VMEM((rows, head // 2), jnp.int32),
            pltpu.SemaphoreType.DMA((4,)), pltpu.SemaphoreType.DMA((3, width // KSTEP)), pltpu.SemaphoreType.DMA((2, groups)), pltpu.SemaphoreType.DMA((2, groups)),
        ],
        compiler_params=pltpu.CompilerParams(vmem_limit_bytes=66_000_000),
        name="attend",
    )(tokens, positions, freq, gain, w_q, w_k, w_v, cache_k, cache_v)


MESH_ID = pl.DeviceIdType.MESH
CHUNK = 1024
SUB = 512
CORES = 2


def finish_kernel(sp_size, tp_size, part_ref, tok_hbm, gain_hbm, wo_hbm, wg_hbm, wu_hbm, wd_hbm, out_ref,
                  tok_ref, gain_ref, wo, wg, wu, wd, crecv, att, dsend, drecv, hbuf, hflat, normed, ubuf, gsum, grecv, obuf,
                  wsem, csem, dsem, hsem, qsem, gsem, asem, bsem, psem):
    f32, bf = jnp.float32, jnp.bfloat16
    rows, width = tok_hbm.shape
    n_x = sp_size // CORES
    heads_cols = wo.shape[0]
    mlp_cols = wg.shape[1]
    sp, tp = lax.axis_index("sp"), lax.axis_index("tp")
    x, core = sp // CORES, sp % CORES
    flip = 1 - core
    group = rows // sp_size

    def rc(src, dst, ssem, rsem, to_sp, to_tp):
        return pltpu.make_async_remote_copy(src_ref=src, dst_ref=dst, send_sem=ssem, recv_sem=rsem,
                                            device_id={"sp": to_sp, "tp": to_tp}, device_id_type=MESH_ID)

    cols = pl.ds(pl.multiple_of(core * mlp_cols, 128), mlp_cols)
    half_width = width // CORES
    out_cols = pl.ds(pl.multiple_of(core * half_width, 128), half_width)
    loads = [pltpu.make_async_copy(wo_hbm, wo.at[:, pl.ds(0, width)], wsem.at[0]),
             pltpu.make_async_copy(wg_hbm.at[:, cols], wg, wsem.at[1]),
             pltpu.make_async_copy(wu_hbm.at[:, cols], wu, wsem.at[2]),
             pltpu.make_async_copy(wd_hbm.at[cols, out_cols], wd.at[0, :, pl.ds(0, half_width)], wsem.at[3]),
             pltpu.make_async_copy(gain_hbm, gain_ref, wsem.at[4]),
             pltpu.make_async_copy(wd_hbm.at[pl.ds(pl.multiple_of(flip * mlp_cols, 128), mlp_cols), out_cols], wd.at[1, :, pl.ds(0, half_width)], wsem.at[6])]
    whole, rest = divmod(width, CHUNK)

    def tokens_chunk(act):
        def run(w):
            src = tok_hbm.at[pl.ds(pl.multiple_of(sp * group, group), group), pl.ds(pl.multiple_of(tp * CHUNK, CHUNK), w)]
            act(pltpu.make_async_copy(src, tok_ref.at[:, pl.ds(0, w)], wsem.at[5]))

        pl.when(tp < whole)(lambda: run(CHUNK))
        if rest:
            pl.when(tp == whole)(lambda: run(rest))

    tokens_chunk(lambda cp: cp.start())
    loads[4].start()
    loads[0].start()
    pending = []

    def send(copy, *args):
        copy(*args).start()
        pending.append(lambda: copy(*args).wait_send())

    barrier = pltpu.get_barrier_semaphore()
    for k in range(1, sp_size):
        pl.semaphore_signal(barrier, inc=1, device_id={"sp": (sp + k) % sp_size, "tp": tp}, device_id_type=MESH_ID)
    for k in range(1, tp_size):
        pl.semaphore_signal(barrier, inc=1, device_id={"sp": sp, "tp": (tp + k) % tp_size}, device_id_type=MESH_ID)
    pl.semaphore_wait(barrier, sp_size + tp_size - 2)

    def part_copy(k):
        to = (sp + k) % sp_size
        return rc(part_ref.at[to], crecv.at[sp], csem.at[0, k - 1], csem.at[1, k - 1], to, tp)

    for k in sorted(range(1, sp_size), key=lambda k: abs(k - sp_size // 2)):
        send(part_copy, k)
    pad = CHUNK * tp_size - width
    wo[:, width:] = jnp.zeros((heads_cols, pad), bf)
    wd[:, :, half_width:] = jnp.zeros((CORES, mlp_cols, SUB * tp_size - half_width), bf)
    if rest:
        @pl.when(tp == whole)
        def _():
            tok_ref[:, rest:] = jnp.zeros((group, CHUNK - rest), bf)
    loads[4].wait()
    tokens_chunk(lambda cp: cp.wait())
    loads[1].start()
    crecv[sp] = part_ref[sp]
    for k in range(1, sp_size):
        src = (sp + sp_size - k) % sp_size
        rc(crecv.at[src], crecv.at[src], csem.at[0, k - 1], csem.at[1, k - 1], sp, tp).wait_recv()

    loads[2].start()
    n_rows = part_ref.shape[1] - 8
    n_pairs = n_rows // 8
    span = 128 // (2 * n_pairs)
    head = part_ref.shape[2]
    heads = heads_cols // head
    stats = [crecv[i, n_rows:, :128] for i in range(sp_size)]
    top = functools.reduce(jnp.maximum, stats)
    factors = [jnp.exp(st - top) for st in stats]
    for j in range(n_pairs):
        lo = 2 * j * span
        num, den = None, None
        for i in range(sp_size):
            f = factors[i][:, lo:lo + 1]
            o = crecv[i, j * 8:(j + 1) * 8, :] * f
            l = stats[i][:, lo + span:lo + span + 1] * f
            num, den = (o, l) if num is None else (num + o, den + l)
        o = num / den
        att[0, j * 8:(j + 1) * 8, :] = o[:, :head // 2]
        att[1, j * 8:(j + 1) * 8, :] = o[:, head // 2:]
    attended = jnp.concatenate([att[half, pl.ds(h, group, stride=heads), :] for h in range(heads) for half in range(2)], axis=-1).astype(bf)

    loads[0].wait()

    def proj_copy(k):
        to = (tp + k) % tp_size
        return rc(dsend.at[to], drecv.at[k - 1], dsem.at[0, k - 1], dsem.at[1, k - 1], sp, to)

    far_first, order = (2, 1, 3), (1, 3, 2)
    for k in far_first + (0,):
        t = (tp + k) % tp_size
        dsend[t] = jnp.dot(attended, wo[:, pl.ds(pl.multiple_of(t * CHUNK, CHUNK), CHUNK)], preferred_element_type=f32)
        if k:
            send(proj_copy, k)
    mine = dsend[tp]
    for k in order:
        rc(drecv.at[k - 1], drecv.at[k - 1], dsem.at[0, k - 1], dsem.at[1, k - 1], sp, tp).wait_recv()
        mine = mine + drecv[k - 1]
    hbuf[core, tp] = (tok_ref[...].astype(f32) + mine).astype(bf).astype(f32)

    loads[3].start()
    loads[5].start()

    partner = sp + 1 - 2 * core

    def h_copy(k):
        return rc(hbuf.at[core, tp], hbuf.at[core, tp], hsem.at[0, k - 1], hsem.at[1, k - 1], sp, (tp + k) % tp_size)

    def q_copy(k):
        t = (tp + tp_size - k) % tp_size
        return rc(hbuf.at[core, t], hbuf.at[core, t], qsem.at[0, k], qsem.at[1, k], partner, tp)

    for k in far_first:
        send(h_copy, k)
    send(q_copy, 0)
    for k in order:
        t = (tp + tp_size - k) % tp_size
        rc(hbuf.at[core, t], hbuf.at[core, t], hsem.at[0, k - 1], hsem.at[1, k - 1], sp, tp).wait_recv()
        send(q_copy, k)
    for k in (0,) + order:
        t = (tp + tp_size - k) % tp_size
        rc(hbuf.at[flip, t], hbuf.at[flip, t], qsem.at[0, k], qsem.at[1, k], sp, tp).wait_recv()

    chip_rows = CORES * group
    square = None
    for t in range(tp_size):
        w = min(CHUNK, width - t * CHUNK)
        v = hbuf[:, t].reshape(chip_rows, CHUNK)[:, :w]
        hflat[:, t * CHUNK:t * CHUNK + w] = v
        s = jnp.sum(v * v, axis=-1, keepdims=True)
        square = s if square is None else square + s
    inv = lax.rsqrt(square / width + NORM_EPS)
    for t in range(tp_size):
        w = min(CHUNK, width - t * CHUNK)
        v = hbuf[:, t].reshape(chip_rows, CHUNK)[:, :w]
        normed[:, t * CHUNK:t * CHUNK + w] = (v * inv * gain_ref[t * CHUNK:t * CHUNK + w].astype(f32).reshape(1, w)).astype(bf)
    loads[1].wait()
    gate = jnp.dot(normed[...], wg[...], preferred_element_type=f32)
    loads[2].wait()
    up = jnp.dot(normed[...], wu[...], preferred_element_type=f32)
    hflat[:, width:] = jnp.zeros((chip_rows, CHUNK * tp_size - width), f32)
    ubuf[core] = (jax.nn.silu(gate) * up).astype(bf).astype(f32)

    def u_copy():
        return rc(ubuf.at[core], ubuf.at[core], qsem.at[0, tp_size], qsem.at[1, tp_size], partner, tp)

    def sum_copy(k):
        return rc(gsum.at[k], grecv.at[k - 1], gsem.at[0, k - 1], gsem.at[1, k - 1], sp, (tp + k) % tp_size)

    send(u_copy)
    steps = far_first + (0,)
    for half in range(CORES):
        if half:
            rc(ubuf.at[flip], ubuf.at[flip], qsem.at[0, tp_size], qsem.at[1, tp_size], sp, tp).wait_recv()
        u = (ubuf[flip] if half else ubuf[core]).astype(bf)
        loads[5 if half else 3].wait()
        for i in steps:
            at = pl.ds(pl.multiple_of((tp + i) % tp_size * SUB, SUB), SUB)
            part = jnp.dot(u, wd[half, :, at], preferred_element_type=f32)
            gsum[i] = gsum[i] + part if half else part
            if half and i:
                send(sum_copy, i)
    acc = gsum[0]
    for k in order:
        rc(grecv.at[k - 1], grecv.at[k - 1], gsem.at[0, k - 1], gsem.at[1, k - 1], sp, tp).wait_recv()
        acc = acc + grecv[k - 1]
    mine = pl.ds(pl.multiple_of(core * half_width + tp * SUB, 128), SUB)
    obuf[x, core, tp] = (hflat[:, mine] + acc).astype(bf).astype(f32)

    def gather(buf):
        def chunk(s, t):
            return buf.at[s // CORES, s % CORES, t]

        def own_chunk(d_sp, d_tp, c, k, j):
            s = (d_sp + sp_size - CORES * (k * (1 - c) + j * c)) % sp_size
            t = (d_tp + tp_size - (k * c + j * (1 - c))) % tp_size
            return s, t

        def first_copy(k):
            return rc(chunk(sp, tp), chunk(sp, tp), asem.at[0, k - 1], asem.at[1, k - 1],
                      (sp + CORES * k * core) % sp_size, (tp + k * flip) % tp_size)

        def second_copy(k, j):
            s, t = own_chunk(sp, tp, core, 0, j)
            return rc(chunk(s, t), chunk(s, t), bsem.at[0, k - 1, j], bsem.at[1, k - 1, j],
                      (sp + CORES * k * flip) % sp_size, (tp + k * core) % tp_size)

        def pair_copy(k, j):
            s, t = own_chunk(sp, tp, core, k, j)
            return rc(chunk(s, t), chunk(s, t), psem.at[0, k, j], psem.at[1, k, j], partner, tp)

        for k in far_first:
            send(first_copy, k)
        for k in far_first:
            send(second_copy, k, 0)
        send(pair_copy, 0, 0)
        for j in order:
            s, t = own_chunk(sp, tp, core, 0, j)
            rc(chunk(s, t), chunk(s, t), asem.at[0, j - 1], asem.at[1, j - 1], sp, tp).wait_recv()
            for k in far_first:
                send(second_copy, k, j)
            send(pair_copy, 0, j)
        for j in (0,) + order:
            for k in order:
                s, t = own_chunk(sp, tp, core, k, j)
                rc(chunk(s, t), chunk(s, t), bsem.at[0, k - 1, j], bsem.at[1, k - 1, j], sp, tp).wait_recv()
                send(pair_copy, k, j)
        for j in (0,) + order:
            for k in (0,) + order:
                s, t = own_chunk(partner, tp, flip, k, j)
                rc(chunk(s, t), chunk(s, t), psem.at[0, k, j], psem.at[1, k, j], sp, tp).wait_recv()

    gather(obuf)

    for c in range(CORES):
        for t in range(tp_size):
            w = min(SUB, half_width - t * SUB)
            lo = c * half_width + t * SUB
            out_ref[:, lo:lo + w] = obuf[:, c, t].reshape(rows, SUB)[:, :w].astype(bf)
    for done in pending:
        done()


def finish(sp_size, tp_size, part, tokens, gain, w_o, w_gate, w_up, w_down):
    rows, width = tokens.shape
    group = rows // sp_size
    n_x = sp_size // CORES
    mlp_cols = w_gate.shape[1] // CORES
    padded = CHUNK * tp_size
    f32, bf = jnp.float32, jnp.bfloat16
    any_spec = pl.BlockSpec(memory_space=pltpu.HBM)
    vm = pl.BlockSpec(memory_space=pltpu.VMEM)
    dma = pltpu.SemaphoreType.DMA
    head = part.shape[2]
    return pl.pallas_call(
        functools.partial(finish_kernel, sp_size, tp_size),
        out_shape=pltpu.VMEM((rows, width), bf),
        in_specs=[vm] + [any_spec] * 6,
        out_specs=vm,
        scratch_shapes=[
            pltpu.VMEM((group, CHUNK), bf), pltpu.VMEM(gain.shape, bf),
            pltpu.VMEM((w_o.shape[0], padded), bf), pltpu.VMEM((width, mlp_cols), bf), pltpu.VMEM((width, mlp_cols), bf), pltpu.VMEM((CORES, mlp_cols, SUB * tp_size), bf),
            pltpu.VMEM(part.shape, f32), pltpu.VMEM((2, part.shape[1] - 8, head // 2), f32),
            pltpu.VMEM((tp_size, group, CHUNK), f32), pltpu.VMEM((tp_size - 1, group, CHUNK), f32),
            pltpu.VMEM((CORES, tp_size, group, CHUNK), f32),
            pltpu.VMEM((CORES * group, padded), f32), pltpu.VMEM((CORES * group, width), bf), pltpu.VMEM((CORES, CORES * group, mlp_cols), f32),
            pltpu.VMEM((tp_size, CORES * group, SUB), f32), pltpu.VMEM((tp_size - 1, CORES * group, SUB), f32),
            pltpu.VMEM((n_x, CORES, tp_size, CORES * group, SUB), f32),
            dma((7,)), dma((2, sp_size - 1)), dma((2, tp_size - 1)), dma((2, tp_size - 1)), dma((2, tp_size + 1)), dma((2, tp_size - 1)),
            dma((2, 3)), dma((2, 3, tp_size)), dma((2, n_x, tp_size)),
        ],
        compiler_params=pltpu.CompilerParams(vmem_limit_bytes=65_500_000, collective_id=0, has_side_effects=True),
        name="finish",
    )(part, tokens, gain, w_o, w_gate, w_up, w_down)


from jax.sharding import PartitionSpec as P


def solution(mesh):
    sp_size, tp_size = mesh.shape["sp"], mesh.shape["tp"]
    cache_spec = P("dp", "sp", "tp", None)
    row_spec = P("dp", None)
    col_spec = P(None, "tp")
    in_specs = (row_spec, P("dp"), cache_spec, cache_spec, P(None), col_spec, col_spec, col_spec, P("tp", None), P(None), col_spec, col_spec, P("tp", None))
    out_specs = (row_spec, cache_spec, cache_spec)

    def local_step(tokens, positions, cache_k, cache_v, attn_gain, w_q, w_k, w_v, w_o, mlp_gain, w_gate, w_up, w_down):
        part, new_k, new_v = attend(sp_size, tokens, positions, cache_k, cache_v, attn_gain, w_q, w_k, w_v)
        part = pltpu.with_memory_space_constraint(part, pltpu.VMEM)
        layer_out = finish(sp_size, tp_size, part, tokens, mlp_gain, w_o, w_gate, w_up, w_down)
        return layer_out, new_k, new_v

    return jax.shard_map(local_step, mesh=mesh, in_specs=in_specs, out_specs=out_specs, check_vma=False)
```

```python
import functools, math
import jax, jax.numpy as jnp, numpy as np
from jax import lax
from jax.experimental import pallas as pl
from jax.experimental.pallas import tpu as pltpu

NORM_EPS = 1e-5
ROPE_THETA = 10000.0
GRP = 8
KSTEP = 768
AHEAD = 3


def attend_kernel(sp_size, tok_hbm, pos_hbm, freq_hbm, gain_hbm, wq_hbm, wk_hbm, wv_hbm, ck_hbm, cv_hbm,
                  part_ref, nk_hbm, nv_hbm,
                  tok_ref, pos_ref, freq_ref, gain_ref, wq, wk, wv, kbuf, vbuf, acc, normed, qrows, knew, vnew, posrow, isem, wsem, csem, osem):
    rows, width = tok_ref.shape
    slots_local = kbuf.shape[1]
    kv_heads = kbuf.shape[2]
    head = kbuf.shape[3]
    q_cols, k_cols = wq.shape[1], wk.shape[1]
    heads = q_cols // head
    half = head // 2
    slots = slots_local * sp_size
    my_first = lax.axis_index("sp") * slots_local
    groups = rows // GRP
    ksteps = width // KSTEP

    def wcopies(c):
        sl = pl.ds(pl.multiple_of(c * KSTEP, KSTEP), KSTEP)
        return [pltpu.make_async_copy(src.at[sl], dst.at[sl], wsem.at[i, c])
                for i, (src, dst) in enumerate(((wq_hbm, wq), (wk_hbm, wk), (wv_hbm, wv)))]

    def ccopies(g):
        sl = pl.ds(g * GRP, GRP)
        return [pltpu.make_async_copy(ck_hbm.at[sl], kbuf.at[sl], csem.at[0, g]),
                pltpu.make_async_copy(cv_hbm.at[sl], vbuf.at[sl], csem.at[1, g])]

    def ocopies(g):
        sl = pl.ds(g * GRP, GRP)
        return [pltpu.make_async_copy(kbuf.at[sl], nk_hbm.at[sl], osem.at[0, g]),
                pltpu.make_async_copy(vbuf.at[sl], nv_hbm.at[sl], osem.at[1, g])]

    inputs = [pltpu.make_async_copy(src, dst, isem.at[i])
              for i, (src, dst) in enumerate(((tok_hbm, tok_ref), (pos_hbm, pos_ref), (freq_hbm, freq_ref), (gain_hbm, gain_ref)))]
    for cp in inputs:
        cp.start()
    for c in range(AHEAD):
        for cp in wcopies(c):
            cp.start()
    for cp in inputs:
        cp.wait()
    wide = tok_ref[...].astype(jnp.float32)
    inv = lax.rsqrt(jnp.mean(wide * wide, axis=-1, keepdims=True) + NORM_EPS)
    normed[...] = (wide * inv * gain_ref[...].astype(jnp.float32).reshape(1, width)).astype(jnp.bfloat16)
    for b in range(rows):
        posrow[b:b + 1, :] = jnp.full((1, half), pos_ref[b], jnp.int32)
    angles = posrow[...].astype(jnp.float32) * freq_ref[...]
    cos, sin = jnp.cos(angles), jnp.sin(angles)
    acc[...] = jnp.zeros_like(acc)

    @pl.loop(0, ksteps)
    def _(c):
        for cp in wcopies(c):
            cp.wait()

        @pl.when(c + AHEAD < ksteps)
        def _():
            for cp in wcopies(c + AHEAD):
                cp.start()

        @pl.when(c + AHEAD >= ksteps)
        def _():
            for cp in ccopies(c + AHEAD - ksteps):
                cp.start()

        sl = pl.ds(pl.multiple_of(c * KSTEP, KSTEP), KSTEP)
        lhs = normed[:, sl]
        for w, off, cols in ((wq, 0, q_cols), (wk, q_cols, k_cols), (wv, q_cols + k_cols, k_cols)):
            acc[:, off:off + cols] += jnp.dot(lhs, w[sl, :], preferred_element_type=jnp.float32)

    def rope(off):
        a = acc[:, off:off + half]
        b = acc[:, off + half:off + head]
        return jnp.concatenate([a * cos - b * sin, b * cos + a * sin], axis=-1)

    for h in range(heads):
        q = rope(h * head).astype(jnp.bfloat16).astype(jnp.float32)
        qrows[0, pl.ds(h, rows, stride=heads), :] = q[:, :half]
        qrows[1, pl.ds(h, rows, stride=heads), :] = q[:, half:]
    for h in range(kv_heads):
        knew[:, h, :] = rope(q_cols + h * head)
        off = q_cols + k_cols + h * head
        vnew[:, h, :] = acc[:, off:off + head]

    pair = 8 // heads
    merged = slots_local * kv_heads
    lane = lax.broadcasted_iota(jnp.int32, (8, merged), 1)
    row = lax.broadcasted_iota(jnp.int32, (8, merged), 0)
    lane_slot = my_first + lane // kv_heads
    same_head = (lane % kv_heads) == ((row % heads) // (heads // kv_heads))
    scale = 1.0 / math.sqrt(head)
    stat_lane = lax.broadcasted_iota(jnp.int32, (8, 128), 1)
    n_pairs = GRP // pair
    span = 128 // (2 * n_pairs)

    @pl.loop(0, groups)
    def _(g):
        for cp in ccopies(g):
            cp.wait()

        @pl.when(g + AHEAD < groups)
        def _():
            for cp in ccopies(g + AHEAD):
                cp.start()

        for i in range(GRP):
            b = g * GRP + i
            local = pos_ref[b] % slots - my_first
            here = (local >= 0) & (local < slots_local)
            at = jnp.clip(local, 0, slots_local - 1)
            for buf, new in ((kbuf, knew), (vbuf, vnew)):
                buf[b, at] = jnp.where(here, new[b], buf[b, at].astype(jnp.float32)).astype(jnp.bfloat16)
        for cp in ocopies(g):
            cp.start()
        stat = jnp.zeros((8, 128), jnp.float32)
        for j in range(n_pairs):
            b0 = g * GRP + j * pair
            q_at = pl.ds(pl.multiple_of(b0 * heads, 8), 8)
            q8 = jnp.concatenate([qrows[0, q_at, :], qrows[1, q_at, :]], axis=-1).astype(jnp.bfloat16)
            s = None
            lim = None
            for i in range(pair):
                kk = kbuf[b0 + i].reshape(merged, head)
                si = lax.dot_general(q8, kk, (((1,), (1,)), ((), ())), preferred_element_type=jnp.float32)
                li = jnp.minimum(pos_ref[b0 + i], slots - 1)
                s = si if s is None else jnp.where(row < i * heads, s, si)
                lim = jnp.full((8, merged), li, jnp.int32) if lim is None else jnp.where(row < i * heads, lim, li)
            valid = same_head & (lane_slot <= lim)
            s = jnp.where(valid, s * scale, -jnp.inf)
            top = jnp.max(s, axis=-1, keepdims=True)
            safe = jnp.where(top == -jnp.inf, 0.0, top)
            p = jnp.exp(s - safe)
            total = jnp.sum(p, axis=-1, keepdims=True)
            out = None
            for i in range(pair):
                vv = vbuf[b0 + i].reshape(merged, head)
                mine = (row >= i * heads) & (row < (i + 1) * heads)
                oi = jnp.dot(jnp.where(mine, p, 0.0).astype(jnp.bfloat16), vv, preferred_element_type=jnp.float32)
                out = oi if out is None else out + oi
            part_ref[g, j * 8:(j + 1) * 8, :] = out
            lo = 2 * j * span
            stat = jnp.where((stat_lane >= lo) & (stat_lane < lo + span), top, stat)
            stat = jnp.where((stat_lane >= lo + span) & (stat_lane < lo + 2 * span), total, stat)
        part_ref[g, n_pairs * 8:, :128] = stat
        part_ref[g, n_pairs * 8:, 128:] = stat

    for g in range(groups):
        for cp in ocopies(g):
            cp.wait()


def attend(sp_size, tokens, positions, cache_k, cache_v, gain, w_q, w_k, w_v):
    rows, width = tokens.shape
    _, slots_local, kv_heads, head = cache_k.shape
    heads = w_q.shape[1] // head
    freq = jnp.asarray((np.float32(ROPE_THETA) ** (np.float32(-2.0) * np.arange(head // 2, dtype=np.float32) / np.float32(head))).astype(np.float32))[None, :]
    groups = rows // GRP
    chunk_rows = GRP * heads + 8
    any_spec = pl.BlockSpec(memory_space=pltpu.HBM)
    vm = pl.BlockSpec(memory_space=pltpu.VMEM)
    qkv_cols = w_q.shape[1] + 2 * w_k.shape[1]
    bf = jnp.bfloat16
    return pl.pallas_call(
        functools.partial(attend_kernel, sp_size),
        out_shape=(pltpu.VMEM((groups, chunk_rows, head), jnp.float32),
                   jax.ShapeDtypeStruct(cache_k.shape, bf), jax.ShapeDtypeStruct(cache_v.shape, bf)),
        in_specs=[any_spec] * 9,
        out_specs=(vm, any_spec, any_spec),
        scratch_shapes=[
            pltpu.VMEM(tokens.shape, bf), pltpu.SMEM(positions.shape, jnp.int32), pltpu.VMEM((1, head // 2), jnp.float32), pltpu.VMEM(gain.shape, bf),
            pltpu.VMEM(w_q.shape, bf), pltpu.VMEM(w_k.shape, bf), pltpu.VMEM(w_v.shape, bf),
            pltpu.VMEM(cache_k.shape, bf), pltpu.VMEM(cache_v.shape, bf),
            pltpu.VMEM((rows, qkv_cols), jnp.float32), pltpu.VMEM((rows, width), bf),
            pltpu.VMEM((2, rows * heads, head // 2), jnp.float32),
            pltpu.VMEM((rows, kv_heads, head), jnp.float32), pltpu.VMEM((rows, kv_heads, head), jnp.float32),
            pltpu.VMEM((rows, head // 2), jnp.int32),
            pltpu.SemaphoreType.DMA((4,)), pltpu.SemaphoreType.DMA((3, width // KSTEP)), pltpu.SemaphoreType.DMA((2, groups)), pltpu.SemaphoreType.DMA((2, groups)),
        ],
        compiler_params=pltpu.CompilerParams(vmem_limit_bytes=66_000_000),
        name="attend",
    )(tokens, positions, freq, gain, w_q, w_k, w_v, cache_k, cache_v)


MESH_ID = pl.DeviceIdType.MESH
CHUNK = 1024
SUB = 512
CORES = 2


def finish_kernel(sp_size, tp_size, part_ref, tok_hbm, gain_hbm, wo_hbm, wg_hbm, wu_hbm, wd_hbm, out_ref,
                  tok_ref, gain_ref, wo, wg, wu, wd, crecv, att, dsend, drecv, hbuf, hflat, normed, ubuf, gsum, grecv, obuf,
                  wsem, csem, dsem, hsem, qsem, gsem, asem, bsem, psem):
    f32, bf = jnp.float32, jnp.bfloat16
    rows, width = tok_hbm.shape
    n_x = sp_size // CORES
    heads_cols = wo.shape[0]
    mlp_cols = wg.shape[1]
    sp, tp = lax.axis_index("sp"), lax.axis_index("tp")
    x, core = sp // CORES, sp % CORES
    flip = 1 - core
    group = rows // sp_size

    def rc(src, dst, ssem, rsem, to_sp, to_tp):
        return pltpu.make_async_remote_copy(src_ref=src, dst_ref=dst, send_sem=ssem, recv_sem=rsem,
                                            device_id={"sp": to_sp, "tp": to_tp}, device_id_type=MESH_ID)

    cols = pl.ds(pl.multiple_of(core * mlp_cols, 128), mlp_cols)
    half_width = width // CORES
    out_cols = pl.ds(pl.multiple_of(core * half_width, 128), half_width)
    loads = [pltpu.make_async_copy(wo_hbm, wo.at[:, pl.ds(0, width)], wsem.at[0]),
             pltpu.make_async_copy(wg_hbm.at[:, cols], wg, wsem.at[1]),
             pltpu.make_async_copy(wu_hbm.at[:, cols], wu, wsem.at[2]),
             pltpu.make_async_copy(wd_hbm.at[cols, out_cols], wd.at[0, :, pl.ds(0, half_width)], wsem.at[3]),
             pltpu.make_async_copy(gain_hbm, gain_ref, wsem.at[4]),
             pltpu.make_async_copy(wd_hbm.at[pl.ds(pl.multiple_of(flip * mlp_cols, 128), mlp_cols), out_cols], wd.at[1, :, pl.ds(0, half_width)], wsem.at[6])]
    whole, rest = divmod(width, CHUNK)

    def tokens_chunk(act):
        def run(w):
            src = tok_hbm.at[pl.ds(pl.multiple_of(sp * group, group), group), pl.ds(pl.multiple_of(tp * CHUNK, CHUNK), w)]
            act(pltpu.make_async_copy(src, tok_ref.at[:, pl.ds(0, w)], wsem.at[5]))

        pl.when(tp < whole)(lambda: run(CHUNK))
        if rest:
            pl.when(tp == whole)(lambda: run(rest))

    tokens_chunk(lambda cp: cp.start())
    loads[4].start()
    loads[0].start()
    pending = []

    def send(copy, *args):
        copy(*args).start()
        pending.append(lambda: copy(*args).wait_send())

    barrier = pltpu.get_barrier_semaphore()
    for k in range(1, sp_size):
        pl.semaphore_signal(barrier, inc=1, device_id={"sp": (sp + k) % sp_size, "tp": tp}, device_id_type=MESH_ID)
    for k in range(1, tp_size):
        pl.semaphore_signal(barrier, inc=1, device_id={"sp": sp, "tp": (tp + k) % tp_size}, device_id_type=MESH_ID)
    pl.semaphore_wait(barrier, sp_size + tp_size - 2)

    def part_copy(k):
        to = (sp + k) % sp_size
        return rc(part_ref.at[to], crecv.at[sp], csem.at[0, k - 1], csem.at[1, k - 1], to, tp)

    for k in sorted(range(1, sp_size), key=lambda k: abs(k - sp_size // 2)):
        send(part_copy, k)
    pad = CHUNK * tp_size - width
    wo[:, width:] = jnp.zeros((heads_cols, pad), bf)
    wd[:, :, half_width:] = jnp.zeros((CORES, mlp_cols, SUB * tp_size - half_width), bf)
    if rest:
        @pl.when(tp == whole)
        def _():
            tok_ref[:, rest:] = jnp.zeros((group, CHUNK - rest), bf)
    loads[4].wait()
    tokens_chunk(lambda cp: cp.wait())
    loads[1].start()
    crecv[sp] = part_ref[sp]
    for k in range(1, sp_size):
        src = (sp + sp_size - k) % sp_size
        rc(crecv.at[src], crecv.at[src], csem.at[0, k - 1], csem.at[1, k - 1], sp, tp).wait_recv()

    loads[2].start()
    n_rows = part_ref.shape[1] - 8
    n_pairs = n_rows // 8
    span = 128 // (2 * n_pairs)
    head = part_ref.shape[2]
    heads = heads_cols // head
    stats = [crecv[i, n_rows:, :128] for i in range(sp_size)]
    top = functools.reduce(jnp.maximum, stats)
    factors = [jnp.exp(st - top) for st in stats]
    for j in range(n_pairs):
        lo = 2 * j * span
        num, den = None, None
        for i in range(sp_size):
            f = factors[i][:, lo:lo + 1]
            o = crecv[i, j * 8:(j + 1) * 8, :] * f
            l = stats[i][:, lo + span:lo + span + 1] * f
            num, den = (o, l) if num is None else (num + o, den + l)
        o = num / den
        att[0, j * 8:(j + 1) * 8, :] = o[:, :head // 2]
        att[1, j * 8:(j + 1) * 8, :] = o[:, head // 2:]
    attended = jnp.concatenate([att[half, pl.ds(h, group, stride=heads), :] for h in range(heads) for half in range(2)], axis=-1).astype(bf)

    loads[0].wait()

    def proj_copy(k):
        to = (tp + k) % tp_size
        return rc(dsend.at[to], drecv.at[k - 1], dsem.at[0, k - 1], dsem.at[1, k - 1], sp, to)

    far_first, order = (2, 1, 3), (1, 3, 2)
    for k in far_first + (0,):
        t = (tp + k) % tp_size
        dsend[t] = jnp.dot(attended, wo[:, pl.ds(pl.multiple_of(t * CHUNK, CHUNK), CHUNK)], preferred_element_type=f32)
        if k:
            send(proj_copy, k)
    mine = dsend[tp]
    for k in order:
        rc(drecv.at[k - 1], drecv.at[k - 1], dsem.at[0, k - 1], dsem.at[1, k - 1], sp, tp).wait_recv()
        mine = mine + drecv[k - 1]
    hbuf[core, tp] = (tok_ref[...].astype(f32) + mine).astype(bf).astype(f32)

    loads[3].start()
    loads[5].start()

    partner = sp + 1 - 2 * core

    def h_copy(k):
        return rc(hbuf.at[core, tp], hbuf.at[core, tp], hsem.at[0, k - 1], hsem.at[1, k - 1], sp, (tp + k) % tp_size)

    def q_copy(k):
        t = (tp + tp_size - k) % tp_size
        return rc(hbuf.at[core, t], hbuf.at[core, t], qsem.at[0, k], qsem.at[1, k], partner, tp)

    for k in far_first:
        send(h_copy, k)
    send(q_copy, 0)
    for k in order:
        t = (tp + tp_size - k) % tp_size
        rc(hbuf.at[core, t], hbuf.at[core, t], hsem.at[0, k - 1], hsem.at[1, k - 1], sp, tp).wait_recv()
        send(q_copy, k)
    for k in (0,) + order:
        t = (tp + tp_size - k) % tp_size
        rc(hbuf.at[flip, t], hbuf.at[flip, t], qsem.at[0, k], qsem.at[1, k], sp, tp).wait_recv()

    chip_rows = CORES * group
    square = None
    for t in range(tp_size):
        w = min(CHUNK, width - t * CHUNK)
        v = hbuf[:, t].reshape(chip_rows, CHUNK)[:, :w]
        hflat[:, t * CHUNK:t * CHUNK + w] = v
        s = jnp.sum(v * v, axis=-1, keepdims=True)
        square = s if square is None else square + s
    inv = lax.rsqrt(square / width + NORM_EPS)
    for t in range(tp_size):
        w = min(CHUNK, width - t * CHUNK)
        v = hbuf[:, t].reshape(chip_rows, CHUNK)[:, :w]
        normed[:, t * CHUNK:t * CHUNK + w] = (v * inv * gain_ref[t * CHUNK:t * CHUNK + w].astype(f32).reshape(1, w)).astype(bf)
    loads[1].wait()
    gate = jnp.dot(normed[...], wg[...], preferred_element_type=f32)
    loads[2].wait()
    up = jnp.dot(normed[...], wu[...], preferred_element_type=f32)
    hflat[:, width:] = jnp.zeros((chip_rows, CHUNK * tp_size - width), f32)
    ubuf[core] = (jax.nn.silu(gate) * up).astype(bf).astype(f32)

    def u_copy():
        return rc(ubuf.at[core], ubuf.at[core], qsem.at[0, tp_size], qsem.at[1, tp_size], partner, tp)

    def sum_copy(k):
        return rc(gsum.at[k], grecv.at[k - 1], gsem.at[0, k - 1], gsem.at[1, k - 1], sp, (tp + k) % tp_size)

    send(u_copy)
    steps = far_first + (0,)
    for half in range(CORES):
        if half:
            rc(ubuf.at[flip], ubuf.at[flip], qsem.at[0, tp_size], qsem.at[1, tp_size], sp, tp).wait_recv()
        u = (ubuf[flip] if half else ubuf[core]).astype(bf)
        loads[5 if half else 3].wait()
        for i in steps:
            at = pl.ds(pl.multiple_of((tp + i) % tp_size * SUB, SUB), SUB)
            part = jnp.dot(u, wd[half, :, at], preferred_element_type=f32)
            gsum[i] = gsum[i] + part if half else part
            if half and i:
                send(sum_copy, i)
    acc = gsum[0]
    for k in order:
        rc(grecv.at[k - 1], grecv.at[k - 1], gsem.at[0, k - 1], gsem.at[1, k - 1], sp, tp).wait_recv()
        acc = acc + grecv[k - 1]
    mine = pl.ds(pl.multiple_of(core * half_width + tp * SUB, 128), SUB)
    obuf[x, core, tp] = (hflat[:, mine] + acc).astype(bf).astype(f32)

    def gather(buf):
        def chunk(s, t):
            return buf.at[s // CORES, s % CORES, t]

        def own_chunk(d_sp, d_tp, c, k, j):
            s = (d_sp + sp_size - CORES * (k * (1 - c) + j * c)) % sp_size
            t = (d_tp + tp_size - (k * c + j * (1 - c))) % tp_size
            return s, t

        def first_copy(k):
            return rc(chunk(sp, tp), chunk(sp, tp), asem.at[0, k - 1], asem.at[1, k - 1],
                      (sp + CORES * k * core) % sp_size, (tp + k * flip) % tp_size)

        def second_copy(k, j):
            s, t = own_chunk(sp, tp, core, 0, j)
            return rc(chunk(s, t), chunk(s, t), bsem.at[0, k - 1, j], bsem.at[1, k - 1, j],
                      (sp + CORES * k * flip) % sp_size, (tp + k * core) % tp_size)

        def pair_copy(k, j):
            s, t = own_chunk(sp, tp, core, k, j)
            return rc(chunk(s, t), chunk(s, t), psem.at[0, k, j], psem.at[1, k, j], partner, tp)

        for k in far_first:
            send(first_copy, k)
        for k in far_first:
            send(second_copy, k, 0)
        send(pair_copy, 0, 0)
        for j in order:
            s, t = own_chunk(sp, tp, core, 0, j)
            rc(chunk(s, t), chunk(s, t), asem.at[0, j - 1], asem.at[1, j - 1], sp, tp).wait_recv()
            for k in far_first:
                send(second_copy, k, j)
            send(pair_copy, 0, j)
        arrivals = sorted(((k, j) for k in order for j in (0,) + order), key=lambda kj: ((kj[0] == 2) + (0, 2, 3, 2)[kj[1]], kj))
        for k, j in arrivals:
            if k:
                s, t = own_chunk(sp, tp, core, k, j)
                rc(chunk(s, t), chunk(s, t), bsem.at[0, k - 1, j], bsem.at[1, k - 1, j], sp, tp).wait_recv()
                send(pair_copy, k, j)
        for j in (0,) + order:
            for k in (0,) + order:
                s, t = own_chunk(partner, tp, flip, k, j)
                rc(chunk(s, t), chunk(s, t), psem.at[0, k, j], psem.at[1, k, j], sp, tp).wait_recv()

    gather(obuf)

    for c in range(CORES):
        for t in range(tp_size):
            w = min(SUB, half_width - t * SUB)
            lo = c * half_width + t * SUB
            out_ref[:, lo:lo + w] = obuf[:, c, t].reshape(rows, SUB)[:, :w].astype(bf)
    for done in pending:
        done()


def finish(sp_size, tp_size, part, tokens, gain, w_o, w_gate, w_up, w_down):
    rows, width = tokens.shape
    group = rows // sp_size
    n_x = sp_size // CORES
    mlp_cols = w_gate.shape[1] // CORES
    padded = CHUNK * tp_size
    f32, bf = jnp.float32, jnp.bfloat16
    any_spec = pl.BlockSpec(memory_space=pltpu.HBM)
    vm = pl.BlockSpec(memory_space=pltpu.VMEM)
    dma = pltpu.SemaphoreType.DMA
    head = part.shape[2]
    return pl.pallas_call(
        functools.partial(finish_kernel, sp_size, tp_size),
        out_shape=pltpu.VMEM((rows, width), bf),
        in_specs=[vm] + [any_spec] * 6,
        out_specs=vm,
        scratch_shapes=[
            pltpu.VMEM((group, CHUNK), bf), pltpu.VMEM(gain.shape, bf),
            pltpu.VMEM((w_o.shape[0], padded), bf), pltpu.VMEM((width, mlp_cols), bf), pltpu.VMEM((width, mlp_cols), bf), pltpu.VMEM((CORES, mlp_cols, SUB * tp_size), bf),
            pltpu.VMEM(part.shape, f32), pltpu.VMEM((2, part.shape[1] - 8, head // 2), f32),
            pltpu.VMEM((tp_size, group, CHUNK), f32), pltpu.VMEM((tp_size - 1, group, CHUNK), f32),
            pltpu.VMEM((CORES, tp_size, group, CHUNK), f32),
            pltpu.VMEM((CORES * group, padded), f32), pltpu.VMEM((CORES * group, width), bf), pltpu.VMEM((CORES, CORES * group, mlp_cols), f32),
            pltpu.VMEM((tp_size, CORES * group, SUB), f32), pltpu.VMEM((tp_size - 1, CORES * group, SUB), f32),
            pltpu.VMEM((n_x, CORES, tp_size, CORES * group, SUB), f32),
            dma((7,)), dma((2, sp_size - 1)), dma((2, tp_size - 1)), dma((2, tp_size - 1)), dma((2, tp_size + 1)), dma((2, tp_size - 1)),
            dma((2, 3)), dma((2, 3, tp_size)), dma((2, n_x, tp_size)),
        ],
        compiler_params=pltpu.CompilerParams(vmem_limit_bytes=65_500_000, collective_id=0, has_side_effects=True),
        name="finish",
    )(part, tokens, gain, w_o, w_gate, w_up, w_down)


from jax.sharding import PartitionSpec as P


def solution(mesh):
    sp_size, tp_size = mesh.shape["sp"], mesh.shape["tp"]
    cache_spec = P("dp", "sp", "tp", None)
    row_spec = P("dp", None)
    col_spec = P(None, "tp")
    in_specs = (row_spec, P("dp"), cache_spec, cache_spec, P(None), col_spec, col_spec, col_spec, P("tp", None), P(None), col_spec, col_spec, P("tp", None))
    out_specs = (row_spec, cache_spec, cache_spec)

    def local_step(tokens, positions, cache_k, cache_v, attn_gain, w_q, w_k, w_v, w_o, mlp_gain, w_gate, w_up, w_down):
        part, new_k, new_v = attend(sp_size, tokens, positions, cache_k, cache_v, attn_gain, w_q, w_k, w_v)
        part = pltpu.with_memory_space_constraint(part, pltpu.VMEM)
        layer_out = finish(sp_size, tp_size, part, tokens, mlp_gain, w_o, w_gate, w_up, w_down)
        return layer_out, new_k, new_v

    return jax.shard_map(local_step, mesh=mesh, in_specs=in_specs, out_specs=out_specs, check_vma=False)
```
